256 devices in a mesh: radial: 64 (over x, z, core), phi: 4 (over y).
Axes of the slice: x: 4, y: 4, z: 8, core: 2. Of those that a mesh axis runs over, the one named last changes fastest.
Arguments:
- conserved: float32 [8, 512, 64, 128], P(None, 'radial', 'phi'), may hold values from -2.5 to 7, as said below
- core_mass: float32 [1], replicated, may hold values from 0.2 to 1
Outputs:
- advanced: float32 [8, 512, 64, 128], P(None, 'radial', 'phi')
- enclosed_mass: float32 [512], P('radial')
The draws below stay inside these ranges and needn't reach their ends.
Inputs may be any that keep to these rules, and one draw needn't show every extreme that they name: conserved[0] (density) lies between 0.4 and 2.5; conserved[4] exceeds (conserved[1]^2 + conserved[2]^2 + conserved[3]^2)/(2 conserved[0]) by at least 0.6; the speeds |conserved[m]/conserved[0]| stay below 1; conserved[5..7] lie between 0 and conserved[0].
All inputs are finite; a program needn't handle non-finite values.
Results may differ from the reference program's by a relative error of at most 0.0003.
Values sent between devices are 32-bit elements; how exact they have to be, the bound alone decides.
A program may use at most 64 MiB of HBM per device.

```python
import math
import jax
import jax.numpy as jnp
from jax import lax

RD = 8
NT = 128
NR = 512
NP = 64


def draw_conserved(key, part):
    subkeys = jax.random.split(key, 12)
    shape = (NR, NP, NT)
    depth = (jnp.arange(NR, dtype=jnp.float32) + 0.5) / NR
    azimuth = (jnp.arange(NP, dtype=jnp.float32) + 0.5) * (2.0 * math.pi / NP)
    centres = jax.random.uniform(subkeys[6], (3,), jnp.float32, 0.0, 1.0)
    heights = jax.random.uniform(subkeys[7], (3,), jnp.float32, -0.13, 0.13)
    bumps = jnp.exp(-jnp.square((depth[:, None] - centres[None, :]) / 0.15))
    profile = jnp.exp(jnp.sum(bumps * heights[None, :], axis=1))
    turn = jax.random.uniform(subkeys[8], (), jnp.float32, 0.0, 2.0 * math.pi)
    twist = jax.random.uniform(subkeys[9], (), jnp.float32, -0.5 * math.pi, 0.5 * math.pi)
    phase = turn + twist * depth
    angular = 1.0 + 0.35 * jnp.cos(azimuth[None, :] - phase[:, None])
    smooth = (profile[:, None] * angular)[:, :, None]
    rough = jnp.exp(jax.random.uniform(subkeys[0], shape, jnp.float32, jnp.log(0.75), jnp.log(1.33)))
    density = jnp.clip(smooth * rough, 0.4, 2.5)
    speeds = [jnp.clip(0.3 * jax.random.normal(subkeys[1 + which], shape, jnp.float32), -0.99, 0.99) for which in range(3)]
    pressure = jax.random.uniform(subkeys[4], shape, jnp.float32, 0.3, 0.9)
    kinetic = 0.5 * density * (speeds[0] * speeds[0] + speeds[1] * speeds[1] + speeds[2] * speeds[2])
    energy = pressure / (4.0 / 3.0 - 1.0) + kinetic
    tracers = jax.random.uniform(subkeys[5], (3,) + shape, jnp.float32, 0.0, 1.0) * density[None]
    momenta = jnp.stack([density * speeds[0], density * speeds[1], density * speeds[2]])
    return jnp.concatenate([density[None], momenta, energy[None], tracers], axis=0)


def setup_inputs(seed: int = 0) -> dict:
    streams_of = jax.random.split(jax.random.key(seed), 3)
    conserved = draw_conserved(jax.random.fold_in(streams_of[2], 71), 0)
    core_mass = jnp.clip(jnp.exp(jax.random.uniform(streams_of[1], (1,), jnp.float32, math.log(0.2), math.log(1.0))), 0.2, 1.0)
    return {"conserved": conserved, "core_mass": core_mass}


ADIABATIC = 4.0 / 3.0
INNER_RADIUS = 1.0
OUTER_RADIUS = 2.0
COURANT = 0.4
GRAVITY_KICK = 0.004
MINIMUM_DENSITY = 0.05
PRESSURE_FLOOR = 0.01

def step_sizes(radial_total, phi_total, theta_total):
    theta_step = math.pi / theta_total
    phi_step = 2.0 * math.pi / phi_total
    polar_width = INNER_RADIUS * math.sin(0.5 * theta_step) * phi_step
    radial_step = min(2.0 * polar_width, (OUTER_RADIUS - INNER_RADIUS) / radial_total)
    timestep = COURANT * min(radial_step, polar_width)
    return (radial_step, theta_step, phi_step, timestep)

def thermo(values):
    density = jnp.maximum(values[0], MINIMUM_DENSITY)
    kinetic = 0.5 * (values[1] * values[1] + values[2] * values[2] + values[3] * values[3]) / density
    pressure = jnp.maximum((ADIABATIC - 1.0) * (values[4] - kinetic), PRESSURE_FLOOR * density)
    return (density, pressure)

def physical(values, component):
    density, pressure = thermo(values)
    normal = values[component] / density
    sound = jnp.sqrt(ADIABATIC * pressure / density)
    pieces = [values[which] * normal for which in range(values.shape[0])]
    pieces[component] = pieces[component] + pressure
    pieces[4] = pieces[4] + pressure * normal
    return (jnp.stack(pieces), jnp.abs(normal) + sound)

def face_flux(values, along_dim, component):
    interior = values.shape[along_dim] - 4
    neighbour_differences = lax.slice_in_dim(values, 1, interior + 4, axis=along_dim) - lax.slice_in_dim(values, 0, interior + 3, axis=along_dim)
    below_diff = lax.slice_in_dim(neighbour_differences, 0, interior + 2, axis=along_dim)
    above_diff = lax.slice_in_dim(neighbour_differences, 1, interior + 3, axis=along_dim)
    limited = 0.5 * (jnp.sign(below_diff) + jnp.sign(above_diff)) * jnp.minimum(jnp.abs(below_diff), jnp.abs(above_diff))
    left_state = lax.slice_in_dim(values, 1, interior + 2, axis=along_dim) + 0.5 * lax.slice_in_dim(limited, 0, interior + 1, axis=along_dim)
    right_state = lax.slice_in_dim(values, 2, interior + 3, axis=along_dim) - 0.5 * lax.slice_in_dim(limited, 1, interior + 2, axis=along_dim)
    left_flux, left_signal = physical(left_state, component)
    right_flux, right_signal = physical(right_state, component)
    signal = jnp.maximum(left_signal, right_signal)
    return 0.5 * (left_flux + right_flux) - 0.5 * signal * (right_state - left_state)

def hydro_rate(extended, cell_centers, enclosed, radial_step, theta_step, phi_step, strength):
    theta_cells = extended.shape[3]
    centre_cells = extended[:, 2:-2, 2:-2, :]
    polar_padded = jnp.pad(centre_cells, ((0, 0), (0, 0), (0, 0), (2, 2)), mode='edge')
    radial_flux = face_flux(extended[:, :, 2:-2, :], 1, 1)
    polar_flux = face_flux(polar_padded, 3, 2)
    azimuth_flux = face_flux(extended[:, 2:-2, :, :], 2, 3)
    angles = (jnp.arange(theta_cells, dtype=jnp.float32) + 0.5) * theta_step
    sine_center = jnp.sin(angles)
    cosine = jnp.cos(angles)
    face_sine = jnp.sin(jnp.arange(theta_cells + 1, dtype=jnp.float32) * theta_step)
    radius = cell_centers[:, None, None]
    face_radius = jnp.concatenate([cell_centers - 0.5 * radial_step, cell_centers[-1:] + 0.5 * radial_step])[:, None, None]
    radial_area = face_radius * face_radius * radial_flux
    divergence = (radial_area[:, 1:] - radial_area[:, :-1]) / (radius * radius * radial_step)
    polar_area = face_sine * polar_flux
    divergence = divergence + (polar_area[..., 1:] - polar_area[..., :-1]) / (radius * sine_center * theta_step)
    divergence = divergence + (azimuth_flux[:, :, 1:] - azimuth_flux[:, :, :-1]) / (radius * sine_center * phi_step)
    density, pressure = thermo(centre_cells)
    radial_speed = centre_cells[1] / density
    polar_speed = centre_cells[2] / density
    azimuth_speed = centre_cells[3] / density
    cotangent = cosine / sine_center
    gravity_pull = strength * enclosed[:, None, None] / (radius * radius)
    source_radial = (2.0 * pressure + density * (polar_speed * polar_speed + azimuth_speed * azimuth_speed)) / radius - density * gravity_pull
    source_polar = (pressure * cotangent + density * azimuth_speed * azimuth_speed * cotangent - density * radial_speed * polar_speed) / radius
    source_azimuth = -density * azimuth_speed * (radial_speed + polar_speed * cotangent) / radius
    source_energy = -centre_cells[1] * gravity_pull
    nothing = jnp.zeros_like(pressure)
    source = jnp.stack([nothing, source_radial, source_polar, source_azimuth, source_energy, nothing, nothing, nothing])
    return source - divergence

def reference(conserved, core_mass):
    radial_total = conserved.shape[1]
    phi_total = conserved.shape[2]
    theta_total = conserved.shape[3]
    radial_step, theta_step, phi_step, timestep = step_sizes(radial_total, phi_total, theta_total)
    strength = GRAVITY_KICK / timestep
    cell_centers = INNER_RADIUS + (jnp.arange(radial_total, dtype=jnp.float32) + 0.5) * radial_step
    sine_center = jnp.sin((jnp.arange(theta_total, dtype=jnp.float32) + 0.5) * theta_step)
    shells = jnp.dot(lax.optimization_barrier(jnp.sum(conserved[0], axis=1)), sine_center, precision=lax.Precision.HIGHEST)
    shells = shells * cell_centers * cell_centers * (radial_step * theta_step * phi_step)
    enclosed = core_mass[0] + jnp.cumsum(shells) - 0.5 * shells
    blocks = radial_total // RD

    def full_rate(values):
        padded = jnp.pad(values, ((0, 0), (2, 2), (0, 0), (0, 0)), mode='edge')
        padded = jnp.pad(padded, ((0, 0), (0, 0), (2, 2), (0, 0)), mode='wrap')

        def one_block(block_index):
            first_row = (block_index * RD).astype(jnp.int32)
            radial_segment = lax.dynamic_slice_in_dim(padded, first_row, RD + 4, 1)
            radius_part = lax.dynamic_slice_in_dim(cell_centers, first_row, RD, 0)
            mass_part = lax.dynamic_slice_in_dim(enclosed, first_row, RD, 0)
            return hydro_rate(radial_segment, radius_part, mass_part, radial_step, theta_step, phi_step, strength)
        stacked = lax.map(one_block, jnp.arange(blocks, dtype=jnp.int32))
        return jnp.transpose(stacked, (1, 0, 2, 3, 4)).reshape(values.shape)
    section_one = conserved + timestep * full_rate(conserved)
    section_two = section_one + timestep * full_rate(section_one)
    advanced = 0.5 * conserved + 0.5 * section_two
    return (advanced, enclosed)
```

```python
import functools
import math

import jax
import jax.numpy as jnp
import numpy as np
from jax import lax
from jax.experimental import pallas as pl
from jax.experimental.pallas import tpu as pltpu
from jax.sharding import PartitionSpec as P

ADIABATIC = 4.0 / 3.0
INNER_RADIUS = 1.0
OUTER_RADIUS = 2.0
COURANT = 0.4
GRAVITY_KICK = 0.004
MINIMUM_DENSITY = 0.05
PRESSURE_FLOOR = 0.01
MESH = pl.DeviceIdType.MESH
TILE = 8
PAD = 8


def step_sizes(radial_total, phi_total, theta_total):
    theta_step = math.pi / theta_total
    phi_step = 2.0 * math.pi / phi_total
    polar_width = INNER_RADIUS * math.sin(0.5 * theta_step) * phi_step
    radial_step = min(2.0 * polar_width, (OUTER_RADIUS - INNER_RADIUS) / radial_total)
    timestep = COURANT * min(radial_step, polar_width)
    return (radial_step, theta_step, phi_step, timestep)


def angle_tables(theta_cells, theta_step):
    step = np.float32(theta_step)
    centre = (np.arange(theta_cells, dtype=np.float32) + np.float32(0.5)) * step
    face = np.arange(theta_cells + 1, dtype=np.float32) * step
    sine = np.sin(centre.astype(np.float64))
    cosine = np.cos(centre.astype(np.float64))
    face_sine = np.sin(face.astype(np.float64))
    face_sine[-1] = 0.0
    zero = np.zeros(theta_cells)
    upper = 0.5 * face_sine[1:] / theta_step
    rows = [sine, upper, cosine / sine, 1.0 / sine, zero, zero, zero, zero]
    return np.stack(rows).astype(np.float32)


def half_slope(below, above):
    high, low = jnp.maximum(below, 0.0), jnp.minimum(below, 0.0)
    return 0.5 * jnp.maximum(jnp.minimum(above, high), low)


def thermo(q):
    density = jnp.maximum(q[0], MINIMUM_DENSITY)
    inverse = 1.0 / density
    kinetic = 0.5 * (q[1] * q[1] + q[2] * q[2] + q[3] * q[3]) * inverse
    pressure = jnp.maximum((ADIABATIC - 1.0) * (q[4] - kinetic), PRESSURE_FLOOR * density)
    return density, inverse, pressure


def physical(q, component):
    _, inverse, pressure = thermo(q)
    normal = q[component] * inverse
    squared = ADIABATIC * pressure * inverse
    return normal, pressure, jnp.abs(normal) + squared * lax.rsqrt(squared)


def flux(left, right, component, half_area):
    left_v, left_p, left_a = physical(left, component)
    right_v, right_p, right_a = physical(right, component)
    signal = jnp.maximum(left_a, right_a)
    left_w = half_area * (left_v + signal)
    right_w = half_area * (right_v - signal)
    out = [a * left_w + b * right_w for a, b in zip(left, right)]
    out[component] = out[component] + half_area * (left_p + right_p)
    out[4] = out[4] + half_area * (left_p * left_v + right_p * right_v)
    return out


def kernel(
    sizes,
    counts,
    core_ref,
    table_ref,
    input_ref,
    out_ref,
    mass_ref,
    first,
    second,
    edge,
    halo,
    radial,
    ends,
    part,
    slab_part,
    got_part,
    got,
    got_above,
    pull,
    table,
    core,
    load_sem,
    radial_send,
    radial_recv,
    phi_send,
    phi_recv,
    part_send,
    part_recv,
    slab_send,
    slab_recv,
    above_send,
    above_recv,
):
    radial_step, theta_step, phi_step, timestep = sizes
    slabs, wedges = counts
    variables, rows, cells, lanes = input_ref.shape
    tiles = cells // TILE
    strength = GRAVITY_KICK / timestep
    slab, wedge = lax.axis_index("radial"), lax.axis_index("phi")
    has_up, has_down = slab < slabs - 1, slab > 0
    shape = (TILE, lanes)

    load = pltpu.make_async_copy(
        input_ref, first.at[:, pl.ds(2, rows), pl.ds(PAD, cells), :], load_sem.at[0]
    )
    load.start()
    load_table = pltpu.make_async_copy(table_ref, table, load_sem.at[1])
    load_table.start()
    load_core = pltpu.make_async_copy(core_ref, core, load_sem.at[2])
    load_core.start()

    def radial_peer(jump):
        return (slab + jump, wedge)

    def phi_peer(jump):
        return (slab, lax.rem(wedge + jump, wedges))

    barrier = pltpu.get_barrier_semaphore()

    def greet(peer):
        pl.semaphore_signal(barrier, inc=1, device_id=peer, device_id_type=MESH)

    for j in range(1, wedges):
        greet(phi_peer(j))

    @pl.when(has_up)
    def _():
        greet(radial_peer(1))

    lax.fori_loop(1, slab + 1, lambda j, _: (greet(radial_peer(-j)), 0)[1], 0)
    greeted = (wedges - 1) + (slabs - 1 - slab) + jnp.where(has_down, 1, 0)

    load.wait()
    load_table.wait()
    load_core.wait()

    def remote(src, dst, send, recv, peer):
        return pltpu.make_async_remote_copy(
            src_ref=src, dst_ref=dst, send_sem=send, recv_sem=recv, device_id=peer,
            device_id_type=MESH,
        )

    def radial_copies(buffer, section):
        where, slot = pl.ds(PAD, cells), 2 * section
        up = remote(
            buffer.at[:, pl.ds(rows, 2), where, :], buffer.at[:, pl.ds(0, 2), where, :],
            radial_send.at[slot], radial_recv.at[slot], radial_peer(1),
        )
        down = remote(
            buffer.at[:, pl.ds(2, 2), where, :], buffer.at[:, pl.ds(rows + 2, 2), where, :],
            radial_send.at[slot + 1], radial_recv.at[slot + 1], radial_peer(-1),
        )
        return up, down

    def radial_start(copies):
        up, down = copies
        pl.when(has_up)(up.start)
        pl.when(has_down)(down.start)

    def radial_sent(copies):
        up, down = copies
        pl.when(has_up)(up.wait_send)
        pl.when(has_down)(down.wait_send)

    def radial_land(copies):
        up, down = copies
        pl.when(has_down)(up.wait_recv)
        pl.when(has_up)(down.wait_recv)

    def radial_ends(buffer):
        for t in range(tiles):
            where = pl.ds(PAD + TILE * t, TILE)

            @pl.when(jnp.logical_not(has_down))
            def _():
                value = buffer[:, 2, where, :]
                buffer[:, 0, where, :] = value
                buffer[:, 1, where, :] = value

            @pl.when(jnp.logical_not(has_up))
            def _():
                value = buffer[:, rows + 1, where, :]
                buffer[:, rows + 2, where, :] = value
                buffer[:, rows + 3, where, :] = value

    def phi_copies(section):
        slot = 2 * section
        return [
            remote(
                edge.at[slot + side], halo.at[slot + side],
                phi_send.at[slot + side], phi_recv.at[slot + side], phi_peer(jump),
            )
            for side, jump in ((0, wedges - 1), (1, 1))
        ]

    def phi_pack(buffer, section):
        for side, start in ((0, PAD), (1, PAD + cells - 2)):
            edge[section * 2 + side] = buffer[:, pl.ds(2, rows), pl.ds(start, 2), :]

    def phi_unpack(buffer, section):
        for side, start in ((0, PAD + cells), (1, PAD - 2)):
            buffer[:, pl.ds(2, rows), pl.ds(start, 2), :] = halo[section * 2 + side]

    lane = lax.broadcasted_iota(jnp.int32, (rows, lanes), 1)
    line = lax.broadcasted_iota(jnp.int32, (rows, lanes), 0)
    column = jnp.sum(first[0, pl.ds(2, rows), pl.ds(PAD, cells), :], axis=1)
    column = jnp.sum(column * table[0:1, :], axis=1, keepdims=True)
    centres = INNER_RADIUS + (
        (slab * rows + line).astype(jnp.float32) + 0.5
    ) * radial_step
    column = column * centres * centres * (radial_step * theta_step * phi_step)
    part[...] = jnp.sum(jnp.where(lane == line, column, 0.0), axis=0, keepdims=True)
    phi_pack(first, 0)

    sub = lax.broadcasted_iota(jnp.int32, shape, 0)
    lane_tile = lax.broadcasted_iota(jnp.int32, shape, 1)
    is_last = lane_tile == lanes - 1
    is_top, is_bottom = sub == TILE - 1, sub == 0

    def spread(value):
        return jnp.broadcast_to(value, shape)

    def radius_of(index):
        index = jnp.full(shape, slab * rows + index, jnp.int32).astype(jnp.float32)
        return INNER_RADIUS + (index + 0.5) * radial_step

    def radial_faces(buffer, low, count, tile):
        where = pl.ds(PAD + TILE * tile, TILE)
        lefts = [[] for _ in range(count)]
        rights = [[] for _ in range(count)]
        for k in range(variables):
            q = [buffer[k, low + j, where, :] for j in range(count + 3)]
            step = [q[j + 1] - q[j] for j in range(count + 2)]
            slope = [half_slope(step[j], step[j + 1]) for j in range(count + 1)]
            for i in range(count):
                lefts[i].append(q[i + 1] + slope[i])
                rights[i].append(q[i + 2] - slope[i + 1])
        out = []
        for i in range(count):
            face = radius_of(low + i) - 0.5 * radial_step
            out.append(flux(lefts[i], rights[i], 1, face * face * (0.5 / radial_step)))
        return out

    def radial_store(buffer, low, count):
        for t in range(tiles):
            for i, face in enumerate(radial_faces(buffer, low, count, t)):
                for k in range(variables):
                    radial[k, low + i, pl.ds(TILE * t, TILE), :] = face[k]

    def theta_part(centre):
        left, right = [], []
        for q in centre:
            after = pltpu.roll(q, lanes - 1, 1)
            above = jnp.where(is_last, 0.0, after - q)
            below = pltpu.roll(above, 1, 1)
            slope = half_slope(below, above)
            left.append(q + slope)
            right.append(pltpu.roll(q - slope, lanes - 1, 1))
        upper = flux(left, right, 2, spread(table[1:2, :]))
        return [pltpu.roll(f, 1, 1) - f for f in upper]

    def phi_ends(buffer):
        def column_at(k, cell):
            return buffer[k, pl.ds(2, rows), PAD + cell, :]

        left, right = [], []
        for k in range(variables):
            a, b, c, d = (column_at(k, cell) for cell in (-2, -1, 0, 1))
            left.append(b + half_slope(b - a, c - b))
            right.append(c - half_slope(c - b, d - c))
            a, b, c = (column_at(k, cell) for cell in (cells - 1, cells, cells + 1))
            ends[1, k] = b - half_slope(b - a, c - b)
        for k, f in enumerate(flux(left, right, 3, 0.5 / phi_step)):
            ends[0, k] = f

    def phi_part(buffer, r):
        left, right = [[] for _ in range(tiles)], [[] for _ in range(tiles)]
        for k in range(variables):
            turned = []
            for t in range(tiles):
                start = PAD + TILE * t
                a, b, c = (
                    buffer[k, r + 2, pl.ds(start + offset, TILE), :] for offset in (-1, 0, 1)
                )
                slope = half_slope(b - a, c - b)
                left[t].append(b + slope)
                turned.append(pltpu.roll(b - slope, TILE - 1, 0))
            turned.append(spread(ends[1, k, pl.ds(r, 1), :]))
            for t in range(tiles):
                right[t].append(jnp.where(is_top, turned[t + 1], turned[t]))
        upper = [flux(left[t], right[t], 3, 0.5 / phi_step) for t in range(tiles)]
        out = [[] for _ in range(tiles)]
        for k in range(variables):
            before = spread(ends[0, k, pl.ds(r, 1), :])
            for t in range(tiles):
                turned = pltpu.roll(upper[t][k], 1, 0)
                out[t].append(jnp.where(is_bottom, before, turned) - upper[t][k])
                before = turned
        return out

    def sources(centre, inverse_r):
        density, inverse, pressure = thermo(centre)
        vr, vt, vp = (centre[m] * inverse for m in (1, 2, 3))
        cot = spread(table[2:3, :])
        swirl = density * vp * vp
        return density, [
            (2.0 * pressure + density * vt * vt + swirl) * inverse_r,
            ((pressure + swirl) * cot - density * vr * vt) * inverse_r,
            -density * vp * (vr + vt * cot) * inverse_r,
        ]

    def centre_at(buffer, r, tile):
        return [
            buffer[k, r + 2, pl.ds(PAD + TILE * tile, TILE), :] for k in range(variables)
        ]

    def early_one(r):
        inverse_r = 1.0 / radius_of(r)
        around = inverse_r * spread(table[3:4, :]) * timestep
        for t in range(tiles):
            centre = centre_at(first, r, t)
            total = [c + d * around for c, d in zip(centre, theta_part(centre))]
            _, source = sources(centre, inverse_r)
            for m in range(3):
                total[m + 1] = total[m + 1] + timestep * source[m]
            for k in range(variables):
                second[k, r + 2, pl.ds(PAD + TILE * t, TILE), :] = total[k]

    def late_one(r):
        inverse_r = 1.0 / radius_of(r)
        around = inverse_r * spread(table[3:4, :]) * timestep
        along = inverse_r * inverse_r * timestep
        for t, part_of in enumerate(phi_part(first, r)):
            into = pl.ds(TILE * t, TILE)
            where = pl.ds(PAD + TILE * t, TILE)
            for k in range(variables):
                across = radial[k, r, into, :] - radial[k, r + 1, into, :]
                second[k, r + 2, where, :] = (
                    second[k, r + 2, where, :] + part_of[k] * around + across * along
                )

    def section_two(r):
        inverse_r = 1.0 / radius_of(r)
        scale = 0.5 * timestep
        around = inverse_r * spread(table[3:4, :]) * scale
        along = inverse_r * inverse_r * scale
        gravity = spread(pull[pl.ds(r + 8, 1), :])
        phi = phi_part(second, r)
        for t in range(tiles):
            into = pl.ds(TILE * t, TILE)
            where = pl.ds(PAD + TILE * t, TILE)
            upper = radial_faces(second, r + 1, 1, t)[0]
            lower = [radial[k, r, into, :] for k in range(variables)]
            for k in range(variables):
                radial[k, r + 1, into, :] = upper[k]
            centre = centre_at(second, r, t)
            theta = theta_part(centre)
            density, source = sources(centre, inverse_r)
            source[0] = source[0] - density * gravity
            source.append(-centre[1] * gravity)
            total = [
                0.5 * (first[k, r + 2, where, :] + centre[k])
                + (theta[k] + phi[t][k]) * around
                + (lower[k] - upper[k]) * along
                for k in range(variables)
            ]
            for m in range(4):
                total[m + 1] = total[m + 1] + scale * source[m]
            for k in range(variables):
                out_ref[k, r, into, :] = total[k]

    def each(low, high, step):
        lax.fori_loop(low, high, lambda r, _: (step(r), 0)[1], 0)

    def each_pair(low, high, step):
        def both(i):
            step(2 * i)
            step(2 * i + 1)

        each(low // 2, high // 2, both)

    each_pair(0, rows, early_one)
    each(0, 2, lambda i: radial_store(first, 2 + 2 * i, 2))
    radial_store(first, 6, 1)

    pl.semaphore_wait(barrier, greeted)

    part_copies = [
        remote(part, got_part.at[j], part_send.at[j], part_recv.at[j], phi_peer(j))
        for j in range(1, wedges)
    ]
    first_radial, second_radial = radial_copies(first, 0), radial_copies(second, 1)
    first_phi, second_phi = phi_copies(0), phi_copies(1)
    for copy in part_copies:
        copy.start()
    radial_start(first_radial)
    for copy in first_phi:
        copy.start()
    got_part[0] = part[...]
    for copy in part_copies:
        copy.wait_recv()
    shells = jnp.zeros((1, lanes), jnp.float32)
    for w in range(wedges):
        shells = shells + got_part[lax.rem(wedge + wedges - w, wedges)]
    slab_part[...] = shells

    def slab_copy(j):
        return remote(
            slab_part, got.at[j], slab_send.at[j], slab_recv.at[j], radial_peer(j)
        )

    above_copy = remote(
        slab_part, got_above, above_send.at[0], above_recv.at[0], radial_peer(-1)
    )
    each(1, slabs - slab, lambda j: slab_copy(j).start())
    pl.when(has_down)(above_copy.start)

    for copy in first_phi:
        copy.wait_recv()
    phi_unpack(first, 0)
    radial_land(first_radial)
    radial_ends(first)
    phi_ends(first)
    each(0, 2, lambda i: radial_store(first, 7 * i, 2))
    each(0, rows, late_one)
    phi_pack(second, 1)
    radial_start(second_radial)
    for copy in second_phi:
        copy.start()

    after = jnp.where(lane < line, 1.0, jnp.where(lane == line, 0.5, 0.0))
    within = jnp.sum(after * slab_part[...], axis=1, keepdims=True)
    whole = jnp.sum(jnp.where(line >= 0, slab_part[...], 0.0), axis=1, keepdims=True)

    for copy in second_phi:
        copy.wait_recv()
    phi_unpack(second, 1)
    radial_land(second_radial)

    radial_sent(second_radial)
    pl.when(has_up)(above_copy.wait_recv)
    each(1, slab + 1, lambda j: slab_copy(j).wait_recv())
    sums = [jnp.zeros((1, lanes), jnp.float32) for _ in range(4)]
    for j in range(1, slabs):
        sums[j % 4] = sums[j % 4] + jnp.where(slab >= j, got[j], 0.0)
    before = jnp.broadcast_to((sums[0] + sums[1]) + (sums[2] + sums[3]), (rows, lanes))
    before = core[0] + jnp.sum(before, axis=1, keepdims=True)
    inner = jnp.where(lane > line, 1.0, jnp.where(lane == line, 0.5, 0.0))
    inner = jnp.sum(inner * got[1], axis=1, keepdims=True)
    outer = jnp.sum(after * got_above[...], axis=1, keepdims=True)
    wide = jnp.zeros((rows, lanes), jnp.float32)
    enclosed = before + within + wide
    mass_ref[...] = jnp.sum(jnp.where(lane == line, enclosed, 0.0), axis=0, keepdims=True)[:, :rows]
    for i, inside in ((0, before - inner), (1, before + within), (2, before + whole + outer)):
        at = centres + (i - 1) * rows * radial_step
        pull[pl.ds(8 * i, 8), :] = strength * (inside + wide) / (at * at)

    def pulled(row, start):
        where = pl.ds(start, TILE)
        gravity = timestep * spread(pull[pl.ds(row + 6, 1), :])
        density = jnp.maximum(first[0, row, where, :], MINIMUM_DENSITY)
        second[1, row, where, :] = second[1, row, where, :] - density * gravity
        second[4, row, where, :] = second[4, row, where, :] - first[1, row, where, :] * gravity

    def pulled_row(row):
        for t in range(-1, tiles + 1):
            pulled(row, PAD + TILE * t)

    each_pair(0, rows + 4, pulled_row)
    radial_ends(second)

    phi_ends(second)
    radial_store(second, 0, 1)
    each(0, rows, section_two)

    for copy in part_copies + first_phi + second_phi:
        copy.wait_send()
    radial_sent(first_radial)
    each(1, slabs - slab, lambda j: slab_copy(j).wait_send())
    pl.when(has_down)(above_copy.wait_send)


def body(conserved, core_mass):
    variables, rows, cells, lanes = conserved.shape
    slabs, wedges = lax.axis_size("radial"), lax.axis_size("phi")
    sizes = step_sizes(rows * slabs, cells * wedges, lanes)
    table = jnp.asarray(angle_tables(lanes, sizes[1]))
    padded = (variables, rows + 4, cells + 2 * PAD, lanes)
    vmem = pl.BlockSpec(memory_space=pltpu.VMEM)
    dma = pltpu.SemaphoreType.DMA
    advanced, mass = pl.pallas_call(
        functools.partial(kernel, sizes, (slabs, wedges)),
        out_shape=(
            pltpu.VMEM(conserved.shape, jnp.float32),
            pltpu.VMEM((1, rows), jnp.float32),
        ),
        in_specs=[pl.BlockSpec(memory_space=pl.ANY)] * 3,
        out_specs=(vmem, vmem),
        scratch_shapes=[
            pltpu.VMEM(padded, jnp.float32),
            pltpu.VMEM(padded, jnp.float32),
            pltpu.VMEM((4, variables, rows, 2, lanes), jnp.float32),
            pltpu.VMEM((4, variables, rows, 2, lanes), jnp.float32),
            pltpu.VMEM((variables, rows + 1, cells, lanes), jnp.float32),
            pltpu.VMEM((2, variables, rows, lanes), jnp.float32),
            pltpu.VMEM((1, lanes), jnp.float32),
            pltpu.VMEM((1, lanes), jnp.float32),
            pltpu.VMEM((wedges, 1, lanes), jnp.float32),
            pltpu.VMEM((slabs, 1, lanes), jnp.float32),
            pltpu.VMEM((1, lanes), jnp.float32),
            pltpu.VMEM((3 * TILE, lanes), jnp.float32),
            pltpu.VMEM((TILE, lanes), jnp.float32),
            pltpu.SMEM((1,), jnp.float32),
            dma((3,)),
            dma((4,)),
            dma((4,)),
            dma((4,)),
            dma((4,)),
            dma((wedges,)),
            dma((wedges,)),
            dma((slabs,)),
            dma((slabs,)),
            dma((1,)),
            dma((1,)),
        ],
        compiler_params=pltpu.CompilerParams(collective_id=0, has_side_effects=True),
    )(core_mass, table, conserved)
    return advanced, mass.reshape(rows)


def solution(mesh):
    in_specs = (P(None, "radial", "phi", None), P())
    out_specs = (P(None, "radial", "phi", None), P("radial"))
    return jax.shard_map(body, mesh=mesh, in_specs=in_specs, out_specs=out_specs, check_vma=False)
```

```python
import functools
import math

import jax
import jax.numpy as jnp
import numpy as np
from jax import lax
from jax.experimental import pallas as pl
from jax.experimental.pallas import tpu as pltpu
from jax.sharding import PartitionSpec as P

ADIABATIC = 4.0 / 3.0
INNER_RADIUS = 1.0
OUTER_RADIUS = 2.0
COURANT = 0.4
GRAVITY_KICK = 0.004
MINIMUM_DENSITY = 0.05
PRESSURE_FLOOR = 0.01
MESH = pl.DeviceIdType.MESH
TILE = 8
PAD = 8
DEPTH = 8
LINE = 2 * DEPTH
TOP = 4


def step_sizes(radial_total, phi_total, theta_total):
    theta_step = math.pi / theta_total
    phi_step = 2.0 * math.pi / phi_total
    polar_width = INNER_RADIUS * math.sin(0.5 * theta_step) * phi_step
    radial_step = min(2.0 * polar_width, (OUTER_RADIUS - INNER_RADIUS) / radial_total)
    timestep = COURANT * min(radial_step, polar_width)
    return (radial_step, theta_step, phi_step, timestep)


def angle_tables(theta_cells, theta_step):
    step = np.float32(theta_step)
    centre = (np.arange(theta_cells, dtype=np.float32) + np.float32(0.5)) * step
    face = np.arange(theta_cells + 1, dtype=np.float32) * step
    sine = np.sin(centre.astype(np.float64))
    cosine = np.cos(centre.astype(np.float64))
    face_sine = np.sin(face.astype(np.float64))
    face_sine[-1] = 0.0
    zero = np.zeros(theta_cells)
    upper = 0.5 * face_sine[1:] / theta_step
    rows = [sine, upper, cosine / sine, 1.0 / sine, zero, zero, zero, zero]
    return np.stack(rows).astype(np.float32)


def half_slope(below, above):
    high, low = jnp.maximum(below, 0.0), jnp.minimum(below, 0.0)
    return 0.5 * jnp.maximum(jnp.minimum(above, high), low)


def thermo(q):
    density = jnp.maximum(q[0], MINIMUM_DENSITY)
    inverse = 1.0 / density
    kinetic = 0.5 * (q[1] * q[1] + q[2] * q[2] + q[3] * q[3]) * inverse
    pressure = jnp.maximum((ADIABATIC - 1.0) * (q[4] - kinetic), PRESSURE_FLOOR * density)
    return density, inverse, pressure


def physical(q, component):
    _, inverse, pressure = thermo(q)
    normal = q[component] * inverse
    squared = ADIABATIC * pressure * inverse
    return normal, pressure, jnp.abs(normal) + squared * lax.rsqrt(squared)


def flux(left, right, component, half_area):
    left_v, left_p, left_a = physical(left, component)
    right_v, right_p, right_a = physical(right, component)
    signal = jnp.maximum(left_a, right_a)
    left_w = half_area * (left_v + signal)
    right_w = half_area * (right_v - signal)
    out = [a * left_w + b * right_w for a, b in zip(left, right)]
    out[component] = out[component] + half_area * (left_p + right_p)
    out[4] = out[4] + half_area * (left_p * left_v + right_p * right_v)
    return out


def kernel(
    sizes,
    counts,
    core_ref,
    table_ref,
    input_ref,
    out_ref,
    mass_ref,
    first,
    second,
    edge,
    halo,
    radial,
    ends,
    part,
    slab_part,
    got_part,
    got,
    got_above,
    pull,
    table,
    core,
    far,
    turn,
    load_sem,
    radial_send,
    radial_recv,
    phi_send,
    phi_recv,
    part_send,
    part_recv,
    slab_send,
    slab_recv,
    above_recv,
):
    radial_step, theta_step, phi_step, timestep = sizes
    slabs, wedges = counts
    variables, rows, cells, lanes = input_ref.shape
    tiles = cells // TILE
    strength = GRAVITY_KICK / timestep
    slab, wedge = lax.axis_index("radial"), lax.axis_index("phi")
    has_up, has_down = slab < slabs - 1, slab > 0
    shape = (TILE, lanes)

    load = pltpu.make_async_copy(
        input_ref, first.at[:, pl.ds(2, rows), pl.ds(PAD, cells), :], load_sem.at[0]
    )
    load.start()
    load_table = pltpu.make_async_copy(table_ref, table, load_sem.at[1])
    load_table.start()
    load_core = pltpu.make_async_copy(core_ref, core, load_sem.at[2])
    load_core.start()

    def radial_peer(jump):
        return (slab + jump, wedge)

    def phi_peer(jump):
        return (slab, lax.rem(wedge + jump, wedges))

    def each(low, high, step):
        lax.fori_loop(low, high, lambda r, _: (step(r), 0)[1], 0)

    barrier = pltpu.get_barrier_semaphore()
    x, z, c = slab // LINE, (slab // 2) % DEPTH, slab % 2
    level = jnp.where(z < TOP, z, TOP + x)
    rank = jnp.where(z < TOP, 2 * x + c, 2 * (z - TOP) + c)
    span, levels = slabs // DEPTH, DEPTH
    turns = jnp.logical_and(slab % LINE == 0, has_down)
    turned_to = jnp.logical_and(slab % LINE == LINE - 1, has_up)
    plain_down = jnp.logical_and(has_down, jnp.logical_not(turns))

    def signal(semaphore, peer):
        pl.semaphore_signal(semaphore, inc=1, device_id=peer, device_id_type=MESH)

    def each_slab(low, high, step):
        def one_level(at):
            for i in range(span):
                spread_out = LINE * (i // 2) + 2 * at + i % 2
                step(jnp.where(at < TOP, spread_out, LINE * (at - TOP) + LINE // 2 + i))

        each(low, high, one_level)

    def greet(v):
        signal(barrier, (v, wedge))

    def greet_level(v):
        pl.when(jnp.logical_or(v < slab, v == slab + 1))(lambda: greet(v))

    for j in range(1, wedges):
        signal(barrier, phi_peer(j))
    pl.when(jnp.logical_and(z > 0, jnp.logical_and(z <= TOP, c == 0)))(lambda: greet(slab - 1))
    each_slab(level, level + 1, greet_level)
    each_slab(level + 1, levels, greet)
    inside = jnp.where(z < TOP, 2 * c, jnp.where(rank > 0, 1, 0))
    greeted = (wedges - 1) + span * level + (span - 1 - rank) + inside
    further = slabs // LINE - 1 - x
    heard = (
        jnp.where(z < TOP, (TOP - 1 - z) * 2 * (further + 1), 0),
        jnp.where(z < TOP, (DEPTH - TOP) * 2 * (further + 1), span * further),
    )

    load.wait()
    load_table.wait()
    load_core.wait()

    def remote(src, dst, send, recv, peer):
        return pltpu.make_async_remote_copy(
            src_ref=src, dst_ref=dst, send_sem=send, recv_sem=recv, device_id=peer,
            device_id_type=MESH,
        )

    def radial_copies(buffer, section):
        where, slot = pl.ds(PAD, cells), 2 * section
        up = remote(
            buffer.at[:, pl.ds(rows, 2), where, :], buffer.at[:, pl.ds(0, 2), where, :],
            radial_send.at[0], radial_recv.at[slot], radial_peer(1),
        )
        down = remote(
            buffer.at[:, pl.ds(2, 2), where, :], buffer.at[:, pl.ds(rows + 2, 2), where, :],
            radial_send.at[1], radial_recv.at[slot + 1], radial_peer(-1),
        )
        return up, down

    def radial_start(copies):
        up, down = copies
        pl.when(has_up)(up.start)
        pl.when(plain_down)(down.start)

    def radial_sent(copies):
        up, down = copies
        pl.when(has_up)(up.wait_send)
        pl.when(has_down)(down.wait_send)

    def radial_land(copies):
        up, down = copies
        pl.when(has_down)(up.wait_recv)
        pl.when(has_up)(down.wait_recv)

    def radial_ends(buffer):
        for t in range(tiles):
            where = pl.ds(PAD + TILE * t, TILE)

            @pl.when(jnp.logical_not(has_down))
            def _():
                value = buffer[:, 2, where, :]
                buffer[:, 0, where, :] = value
                buffer[:, 1, where, :] = value

            @pl.when(jnp.logical_not(has_up))
            def _():
                value = buffer[:, rows + 1, where, :]
                buffer[:, rows + 2, where, :] = value
                buffer[:, rows + 3, where, :] = value

    def phi_copies(section):
        slot = 2 * section
        return [
            remote(
                edge.at[slot + side], halo.at[slot + side],
                phi_send.at[section], phi_recv.at[section], phi_peer(jump),
            )
            for side, jump in ((0, wedges - 1), (1, 1))
        ]

    def phi_both(section):
        slots = pl.ds(2 * section, 2)
        return remote(
            edge.at[slots], halo.at[slots], phi_send.at[section], phi_recv.at[section],
            phi_peer(1),
        )

    def phi_pack(buffer, section):
        for side, start in ((0, PAD), (1, PAD + cells - 2)):
            edge[section * 2 + side] = buffer[:, pl.ds(2, rows), pl.ds(start, 2), :]

    def phi_unpack(buffer, section):
        for side, start in ((0, PAD + cells), (1, PAD - 2)):
            buffer[:, pl.ds(2, rows), pl.ds(start, 2), :] = halo[section * 2 + side]

    lane = lax.broadcasted_iota(jnp.int32, (rows, lanes), 1)
    line = lax.broadcasted_iota(jnp.int32, (rows, lanes), 0)
    column = jnp.sum(first[0, pl.ds(2, rows), pl.ds(PAD, cells), :], axis=1)
    column = jnp.sum(column * table[0:1, :], axis=1, keepdims=True)
    centres = INNER_RADIUS + (
        (slab * rows + line).astype(jnp.float32) + 0.5
    ) * radial_step
    column = column * centres * centres * (radial_step * theta_step * phi_step)
    part[...] = jnp.sum(jnp.where(lane == line, column, 0.0), axis=0, keepdims=True)
    phi_pack(first, 0)

    sub = lax.broadcasted_iota(jnp.int32, shape, 0)
    lane_tile = lax.broadcasted_iota(jnp.int32, shape, 1)
    is_last = lane_tile == lanes - 1
    is_top, is_bottom = sub == TILE - 1, sub == 0

    def spread(value):
        return jnp.broadcast_to(value, shape)

    def radius_of(index):
        index = jnp.full(shape, slab * rows + index, jnp.int32).astype(jnp.float32)
        return INNER_RADIUS + (index + 0.5) * radial_step

    def radial_faces(buffer, low, count, tile):
        where = pl.ds(PAD + TILE * tile, TILE)
        lefts = [[] for _ in range(count)]
        rights = [[] for _ in range(count)]
        for k in range(variables):
            q = [buffer[k, low + j, where, :] for j in range(count + 3)]
            step = [q[j + 1] - q[j] for j in range(count + 2)]
            slope = [half_slope(step[j], step[j + 1]) for j in range(count + 1)]
            for i in range(count):
                lefts[i].append(q[i + 1] + slope[i])
                rights[i].append(q[i + 2] - slope[i + 1])
        out = []
        for i in range(count):
            face = radius_of(low + i) - 0.5 * radial_step
            out.append(flux(lefts[i], rights[i], 1, face * face * (0.5 / radial_step)))
        return out

    def radial_store(buffer, low, count):
        for t in range(tiles):
            for i, face in enumerate(radial_faces(buffer, low, count, t)):
                for k in range(variables):
                    radial[k, low + i, pl.ds(TILE * t, TILE), :] = face[k]

    def theta_part(centre):
        left, right = [], []
        for q in centre:
            after = pltpu.roll(q, lanes - 1, 1)
            above = jnp.where(is_last, 0.0, after - q)
            below = pltpu.roll(above, 1, 1)
            slope = half_slope(below, above)
            left.append(q + slope)
            right.append(pltpu.roll(q - slope, lanes - 1, 1))
        upper = flux(left, right, 2, spread(table[1:2, :]))
        return [pltpu.roll(f, 1, 1) - f for f in upper]

    def phi_ends(buffer):
        def column_at(k, cell):
            return buffer[k, pl.ds(2, rows), PAD + cell, :]

        left, right = [], []
        for k in range(variables):
            a, b, c, d = (column_at(k, cell) for cell in (-2, -1, 0, 1))
            left.append(b + half_slope(b - a, c - b))
            right.append(c - half_slope(c - b, d - c))
            a, b, c = (column_at(k, cell) for cell in (cells - 1, cells, cells + 1))
            ends[1, k] = b - half_slope(b - a, c - b)
        for k, f in enumerate(flux(left, right, 3, 0.5 / phi_step)):
            ends[0, k] = f

    def phi_part(buffer, r):
        left, right = [[] for _ in range(tiles)], [[] for _ in range(tiles)]
        for k in range(variables):
            turned = []
            for t in range(tiles):
                start = PAD + TILE * t
                a, b, c = (
                    buffer[k, r + 2, pl.ds(start + offset, TILE), :] for offset in (-1, 0, 1)
                )
                slope = half_slope(b - a, c - b)
                left[t].append(b + slope)
                turned.append(pltpu.roll(b - slope, TILE - 1, 0))
            turned.append(spread(ends[1, k, pl.ds(r, 1), :]))
            for t in range(tiles):
                right[t].append(jnp.where(is_top, turned[t + 1], turned[t]))
        upper = [flux(left[t], right[t], 3, 0.5 / phi_step) for t in range(tiles)]
        out = [[] for _ in range(tiles)]
        for k in range(variables):
            before = spread(ends[0, k, pl.ds(r, 1), :])
            for t in range(tiles):
                turned = pltpu.roll(upper[t][k], 1, 0)
                out[t].append(jnp.where(is_bottom, before, turned) - upper[t][k])
                before = turned
        return out

    def sources(centre, inverse_r):
        density, inverse, pressure = thermo(centre)
        vr, vt, vp = (centre[m] * inverse for m in (1, 2, 3))
        cot = spread(table[2:3, :])
        swirl = density * vp * vp
        return density, [
            (2.0 * pressure + density * vt * vt + swirl) * inverse_r,
            ((pressure + swirl) * cot - density * vr * vt) * inverse_r,
            -density * vp * (vr + vt * cot) * inverse_r,
        ]

    def centre_at(buffer, r, tile):
        return [
            buffer[k, r + 2, pl.ds(PAD + TILE * tile, TILE), :] for k in range(variables)
        ]

    def early_one(r):
        inverse_r = 1.0 / radius_of(r)
        around = inverse_r * spread(table[3:4, :]) * timestep
        for t in range(tiles):
            centre = centre_at(first, r, t)
            total = [c + d * around for c, d in zip(centre, theta_part(centre))]
            _, source = sources(centre, inverse_r)
            for m in range(3):
                total[m + 1] = total[m + 1] + timestep * source[m]
            for k in range(variables):
                second[k, r + 2, pl.ds(PAD + TILE * t, TILE), :] = total[k]

    def late_one(r):
        inverse_r = 1.0 / radius_of(r)
        around = inverse_r * spread(table[3:4, :]) * timestep
        along = inverse_r * inverse_r * timestep
        for t, part_of in enumerate(phi_part(first, r)):
            into = pl.ds(TILE * t, TILE)
            where = pl.ds(PAD + TILE * t, TILE)
            for k in range(variables):
                across = radial[k, r, into, :] - radial[k, r + 1, into, :]
                second[k, r + 2, where, :] = (
                    second[k, r + 2, where, :] + part_of[k] * around + across * along
                )

    def section_two(r):
        inverse_r = 1.0 / radius_of(r)
        scale = 0.5 * timestep
        around = inverse_r * spread(table[3:4, :]) * scale
        along = inverse_r * inverse_r * scale
        gravity = spread(pull[pl.ds(r + 8, 1), :])
        phi = phi_part(second, r)
        for t in range(tiles):
            into = pl.ds(TILE * t, TILE)
            where = pl.ds(PAD + TILE * t, TILE)
            upper = radial_faces(second, r + 1, 1, t)[0]
            lower = [radial[k, r, into, :] for k in range(variables)]
            for k in range(variables):
                radial[k, r + 1, into, :] = upper[k]
            centre = centre_at(second, r, t)
            theta = theta_part(centre)
            density, source = sources(centre, inverse_r)
            source[0] = source[0] - density * gravity
            source.append(-centre[1] * gravity)
            total = [
                0.5 * (first[k, r + 2, where, :] + centre[k])
                + (theta[k] + phi[t][k]) * around
                + (lower[k] - upper[k]) * along
                for k in range(variables)
            ]
            for m in range(4):
                total[m + 1] = total[m + 1] + scale * source[m]
            for k in range(variables):
                out_ref[k, r, into, :] = total[k]

    def each_pair(low, high, step):
        def both(i):
            step(2 * i)
            step(2 * i + 1)

        each(low // 2, high // 2, both)

    pl.semaphore_wait(barrier, greeted)
    pl.when(turned_to)(lambda: signal(turn, radial_peer(1)))

    def reply(v):
        pl.when(v < slab)(lambda: signal(far.at[jnp.where(z < TOP, 0, 1)], (v, wedge)))

    part_copies = [
        remote(part, got_part.at[j], part_send.at[0], part_recv.at[0], phi_peer(j))
        for j in range(1, wedges)
    ]
    others = pl.ds(1, wedges - 1)
    part_all = remote(
        got_part.at[others], got_part.at[others], part_send.at[0], part_recv.at[0], phi_peer(1)
    )
    first_radial, second_radial = radial_copies(first, 0), radial_copies(second, 1)
    first_phi, second_phi = phi_copies(0), phi_copies(1)
    for copy in part_copies:
        copy.start()
    radial_start(first_radial)
    for copy in first_phi:
        copy.start()
    each_slab(0, level, reply)
    got_part[0] = part[...]
    each_pair(0, rows, early_one)
    each(0, 2, lambda i: radial_store(first, 2 + 2 * i, 2))
    radial_store(first, 6, 1)
    part_all.wait_recv()
    shells = jnp.zeros((1, lanes), jnp.float32)
    for w in range(wedges):
        shells = shells + got_part[lax.rem(wedge + wedges - w, wedges)]
    slab_part[...] = shells

    def slab_copy(source, target):
        return remote(
            slab_part, got.at[source], slab_send.at[0], slab_recv.at[0], (target, wedge),
        )

    def slab_all(count):
        ref = got.at[pl.ds(0, count)]
        return remote(ref, ref, slab_send.at[0], slab_recv.at[0], radial_peer(0))

    def by_slab(low, high, step):
        if high - low == 1:
            step(low)
            return
        middle = (low + high) // 2
        pl.when(slab < middle)(lambda: by_slab(low, middle, step))
        pl.when(slab >= middle)(lambda: by_slab(middle, high, step))

    def slab_start(v):
        pl.when(v > slab)(lambda: slab_copy(slab, v).start())

    above_copy = remote(
        slab_part, got_above, slab_send.at[0], above_recv.at[0], radial_peer(-1)
    )
    each_slab(0, level + 1, slab_start)
    pl.when(plain_down)(above_copy.start)

    @pl.when(turns)
    def _():
        pl.semaphore_wait(turn, 1)
        first_radial[1].start()
        above_copy.start()

    def send_out():
        for at in range(2):
            @pl.when(heard[at] > 0)
            def _():
                pl.semaphore_wait(far.at[at], heard[at])

        each_slab(level + 1, levels, slab_start)

    phi_both(0).wait_recv()
    phi_unpack(first, 0)
    pl.when(turns)(send_out)
    radial_land(first_radial)
    radial_ends(first)
    phi_ends(first)
    each(0, 2, lambda i: radial_store(first, 7 * i, 2))
    each(0, 4, lambda i: late_one(i + (i // 2) * (rows - 4)))
    radial_sent(first_radial)
    radial_start(second_radial)
    pl.when(turns)(second_radial[1].start)
    each(2, rows - 2, late_one)
    phi_pack(second, 1)
    for copy in second_phi:
        copy.start()

    pl.when(jnp.logical_not(turns))(send_out)

    after = jnp.where(lane < line, 1.0, jnp.where(lane == line, 0.5, 0.0))
    within = jnp.sum(after * slab_part[...], axis=1, keepdims=True)
    whole = jnp.sum(jnp.where(line >= 0, slab_part[...], 0.0), axis=1, keepdims=True)

    phi_both(1).wait_recv()
    phi_unpack(second, 1)
    radial_land(second_radial)

    part_all.wait_send()
    phi_both(0).wait_send()
    phi_both(1).wait_send()
    radial_sent(second_radial)
    by_slab(0, slabs, lambda s: slab_all(slabs - max(s, 1)).wait_send())
    pl.when(has_up)(above_copy.wait_recv)
    by_slab(0, slabs, lambda s: slab_all(s).wait_recv() if s else None)
    sums = [jnp.zeros((1, lanes), jnp.float32) for _ in range(4)]
    for v in range(slabs - 1):
        sums[v % 4] = sums[v % 4] + jnp.where(slab > v, got[v], 0.0)
    before = jnp.broadcast_to((sums[0] + sums[1]) + (sums[2] + sums[3]), (rows, lanes))
    before = core[0] + jnp.sum(before, axis=1, keepdims=True)
    inner = jnp.where(lane > line, 1.0, jnp.where(lane == line, 0.5, 0.0))
    inner = jnp.sum(inner * got[jnp.maximum(slab - 1, 0)], axis=1, keepdims=True)
    outer = jnp.sum(after * got_above[...], axis=1, keepdims=True)
    wide = jnp.zeros((rows, lanes), jnp.float32)
    enclosed = before + within + wide
    mass_ref[...] = jnp.sum(jnp.where(lane == line, enclosed, 0.0), axis=0, keepdims=True)[:, :rows]
    for i, inside in ((0, before - inner), (1, before + within), (2, before + whole + outer)):
        at = centres + (i - 1) * rows * radial_step
        pull[pl.ds(8 * i, 8), :] = strength * (inside + wide) / (at * at)

    def pulled(row, start):
        where = pl.ds(start, TILE)
        gravity = timestep * spread(pull[pl.ds(row + 6, 1), :])
        density = jnp.maximum(first[0, row, where, :], MINIMUM_DENSITY)
        second[1, row, where, :] = second[1, row, where, :] - density * gravity
        second[4, row, where, :] = second[4, row, where, :] - first[1, row, where, :] * gravity

    def pulled_row(row):
        for t in range(-1, tiles + 1):
            pulled(row, PAD + TILE * t)

    each_pair(0, rows + 4, pulled_row)
    radial_ends(second)

    phi_ends(second)
    radial_store(second, 0, 1)
    each(0, rows, section_two)


def body(conserved, core_mass):
    variables, rows, cells, lanes = conserved.shape
    slabs, wedges = lax.axis_size("radial"), lax.axis_size("phi")
    sizes = step_sizes(rows * slabs, cells * wedges, lanes)
    table = jnp.asarray(angle_tables(lanes, sizes[1]))
    padded = (variables, rows + 4, cells + 2 * PAD, lanes)
    vmem = pl.BlockSpec(memory_space=pltpu.VMEM)
    dma = pltpu.SemaphoreType.DMA
    advanced, mass = pl.pallas_call(
        functools.partial(kernel, sizes, (slabs, wedges)),
        out_shape=(
            pltpu.VMEM(conserved.shape, jnp.float32),
            pltpu.VMEM((1, rows), jnp.float32),
        ),
        in_specs=[pl.BlockSpec(memory_space=pl.ANY)] * 3,
        out_specs=(vmem, vmem),
        scratch_shapes=[
            pltpu.VMEM(padded, jnp.float32),
            pltpu.VMEM(padded, jnp.float32),
            pltpu.VMEM((4, variables, rows, 2, lanes), jnp.float32),
            pltpu.VMEM((4, variables, rows, 2, lanes), jnp.float32),
            pltpu.VMEM((variables, rows + 1, cells, lanes), jnp.float32),
            pltpu.VMEM((2, variables, rows, lanes), jnp.float32),
            pltpu.VMEM((1, lanes), jnp.float32),
            pltpu.VMEM((1, lanes), jnp.float32),
            pltpu.VMEM((wedges, 1, lanes), jnp.float32),
            pltpu.VMEM((slabs, 1, lanes), jnp.float32),
            pltpu.VMEM((1, lanes), jnp.float32),
            pltpu.VMEM((3 * TILE, lanes), jnp.float32),
            pltpu.VMEM((TILE, lanes), jnp.float32),
            pltpu.SMEM((1,), jnp.float32),
            pltpu.SemaphoreType.REGULAR((2,)),
            pltpu.SemaphoreType.REGULAR,
            dma((3,)),
            dma((2,)),
            dma((4,)),
            dma((2,)),
            dma((2,)),
            dma((1,)),
            dma((1,)),
            dma((1,)),
            dma((1,)),
            dma((1,)),
        ],
        compiler_params=pltpu.CompilerParams(collective_id=0, has_side_effects=True),
    )(core_mass, table, conserved)
    return advanced, mass.reshape(rows)


def solution(mesh):
    in_specs = (P(None, "radial", "phi", None), P())
    out_specs = (P(None, "radial", "phi", None), P("radial"))
    return jax.shard_map(body, mesh=mesh, in_specs=in_specs, out_specs=out_specs, check_vma=False)
```

```python
import functools
import math

import jax
import jax.numpy as jnp
import numpy as np
from jax import lax
from jax.experimental import pallas as pl
from jax.experimental.pallas import tpu as pltpu
from jax.sharding import PartitionSpec as P

ADIABATIC = 4.0 / 3.0
INNER_RADIUS = 1.0
OUTER_RADIUS = 2.0
COURANT = 0.4
GRAVITY_KICK = 0.004
MINIMUM_DENSITY = 0.05
PRESSURE_FLOOR = 0.01
MESH = pl.DeviceIdType.MESH
TILE = 8
PAD = 8
DEPTH = 8
LINE = 2 * DEPTH
TOP = 4


def step_sizes(radial_total, phi_total, theta_total):
    theta_step = math.pi / theta_total
    phi_step = 2.0 * math.pi / phi_total
    polar_width = INNER_RADIUS * math.sin(0.5 * theta_step) * phi_step
    radial_step = min(2.0 * polar_width, (OUTER_RADIUS - INNER_RADIUS) / radial_total)
    timestep = COURANT * min(radial_step, polar_width)
    return (radial_step, theta_step, phi_step, timestep)


def angle_tables(theta_cells, theta_step):
    step = np.float32(theta_step)
    centre = (np.arange(theta_cells, dtype=np.float32) + np.float32(0.5)) * step
    face = np.arange(theta_cells + 1, dtype=np.float32) * step
    sine = np.sin(centre.astype(np.float64))
    cosine = np.cos(centre.astype(np.float64))
    face_sine = np.sin(face.astype(np.float64))
    face_sine[-1] = 0.0
    zero = np.zeros(theta_cells)
    upper = 0.5 * face_sine[1:] / theta_step
    rows = [sine, upper, cosine / sine, 1.0 / sine, zero, zero, zero, zero]
    return np.stack(rows).astype(np.float32)


def half_slope(below, above):
    high, low = jnp.maximum(below, 0.0), jnp.minimum(below, 0.0)
    return 0.5 * jnp.maximum(jnp.minimum(above, high), low)


def thermo(q):
    density = jnp.maximum(q[0], MINIMUM_DENSITY)
    inverse = 1.0 / density
    kinetic = 0.5 * (q[1] * q[1] + q[2] * q[2] + q[3] * q[3]) * inverse
    pressure = jnp.maximum((ADIABATIC - 1.0) * (q[4] - kinetic), PRESSURE_FLOOR * density)
    return density, inverse, pressure


def physical(q, component):
    _, inverse, pressure = thermo(q)
    normal = q[component] * inverse
    squared = ADIABATIC * pressure * inverse
    return normal, pressure, jnp.abs(normal) + squared * lax.rsqrt(squared)


def flux(left, right, component, half_area):
    left_v, left_p, left_a = physical(left, component)
    right_v, right_p, right_a = physical(right, component)
    signal = jnp.maximum(left_a, right_a)
    left_w = half_area * (left_v + signal)
    right_w = half_area * (right_v - signal)
    out = [a * left_w + b * right_w for a, b in zip(left, right)]
    out[component] = out[component] + half_area * (left_p + right_p)
    out[4] = out[4] + half_area * (left_p * left_v + right_p * right_v)
    return out


def kernel(
    sizes,
    counts,
    core_ref,
    table_ref,
    input_ref,
    out_ref,
    mass_ref,
    first,
    second,
    edge,
    halo,
    radial,
    ends,
    part,
    slab_part,
    got_part,
    got,
    got_above,
    pull,
    table,
    core,
    far,
    told,
    load_sem,
    radial_send,
    radial_recv,
    phi_send,
    phi_recv,
    part_send,
    part_recv,
    slab_send,
    slab_recv,
    above_recv,
):
    radial_step, theta_step, phi_step, timestep = sizes
    slabs, wedges = counts
    variables, rows, cells, lanes = input_ref.shape
    tiles = cells // TILE
    strength = GRAVITY_KICK / timestep
    slab, wedge = lax.axis_index("radial"), lax.axis_index("phi")
    has_up, has_down = slab < slabs - 1, slab > 0
    shape = (TILE, lanes)

    load = pltpu.make_async_copy(
        input_ref, first.at[:, pl.ds(2, rows), pl.ds(PAD, cells), :], load_sem.at[0]
    )
    load.start()
    load_table = pltpu.make_async_copy(table_ref, table, load_sem.at[1])
    load_table.start()
    load_core = pltpu.make_async_copy(core_ref, core, load_sem.at[2])
    load_core.start()

    def radial_peer(jump):
        return (slab + jump, wedge)

    def phi_peer(jump):
        return (slab, lax.rem(wedge + jump, wedges))

    def each(low, high, step):
        lax.fori_loop(low, high, lambda r, _: (step(r), 0)[1], 0)

    barrier = pltpu.get_barrier_semaphore()
    x, z, c = slab // LINE, (slab // 2) % DEPTH, slab % 2
    level = jnp.where(z < TOP, z, TOP + x)
    rank = jnp.where(z < TOP, 2 * x + c, 2 * (z - TOP) + c)
    span, levels = slabs // DEPTH, DEPTH
    turns = jnp.logical_and(slab % LINE == 0, has_down)
    turned_last = slab % LINE == LINE - 1
    turned_to = jnp.logical_and(turned_last, has_up)

    def signal(semaphore, peer):
        pl.semaphore_signal(semaphore, inc=1, device_id=peer, device_id_type=MESH)

    def each_slab(low, high, step):
        def one_level(at):
            for i in range(span):
                spread_out = LINE * (i // 2) + 2 * at + i % 2
                step(jnp.where(at < TOP, spread_out, LINE * (at - TOP) + LINE // 2 + i))

        each(low, high, one_level)

    def greet(v):
        signal(barrier, (v, wedge))

    def greet_level(v):
        pl.when(jnp.logical_or(v < slab, v == slab + 1))(lambda: greet(v))

    def greet_outer(v):
        known = jnp.logical_or(v % LINE != LINE - 1, v == slab - 1)
        pl.when(known)(lambda: greet(v))

    for j in range(1, wedges):
        signal(barrier, phi_peer(j))
    pl.when(jnp.logical_and(z > 0, jnp.logical_and(z <= TOP, c == 0)))(lambda: greet(slab - 1))
    pl.when(turned_to)(lambda: greet(slab + 1))
    each_slab(level, level + 1, greet_level)
    each_slab(level + 1, levels, greet_outer)
    inside = jnp.where(z < TOP, 2 * c, jnp.where(rank > 0, 1, 0))
    inside = jnp.where(turned_last, jnp.where(has_up, 2, 1), span * level + span - 1 - rank + inside)
    greeted = (wedges - 1) + inside + jnp.where(turns, 1, 0)
    further = slabs // LINE - 1 - x
    heard = (
        jnp.where(z < TOP, (TOP - 1 - z) * 2 * (further + 1), 0),
        jnp.where(z < TOP, (DEPTH - TOP) * 2 * (further + 1), span * further),
    )

    load.wait()
    load_table.wait()
    load_core.wait()

    def remote(src, dst, send, recv, peer):
        return pltpu.make_async_remote_copy(
            src_ref=src, dst_ref=dst, send_sem=send, recv_sem=recv, device_id=peer,
            device_id_type=MESH,
        )

    def radial_copies(buffer, section):
        where, slot = pl.ds(PAD, cells), 2 * section
        up = remote(
            buffer.at[:, pl.ds(rows, 2), where, :], buffer.at[:, pl.ds(0, 2), where, :],
            radial_send.at[0], radial_recv.at[slot], radial_peer(1),
        )
        down = remote(
            buffer.at[:, pl.ds(2, 2), where, :], buffer.at[:, pl.ds(rows + 2, 2), where, :],
            radial_send.at[1], radial_recv.at[slot + 1], radial_peer(-1),
        )
        return up, down

    def radial_start(copies):
        up, down = copies
        pl.when(has_up)(up.start)
        pl.when(has_down)(down.start)

    def radial_sent(copies):
        up, down = copies
        pl.when(has_up)(up.wait_send)
        pl.when(has_down)(down.wait_send)

    def radial_land(copies):
        up, down = copies
        pl.when(has_down)(up.wait_recv)
        pl.when(has_up)(down.wait_recv)

    def radial_ends(buffer):
        for t in range(tiles):
            where = pl.ds(PAD + TILE * t, TILE)

            @pl.when(jnp.logical_not(has_down))
            def _():
                value = buffer[:, 2, where, :]
                buffer[:, 0, where, :] = value
                buffer[:, 1, where, :] = value

            @pl.when(jnp.logical_not(has_up))
            def _():
                value = buffer[:, rows + 1, where, :]
                buffer[:, rows + 2, where, :] = value
                buffer[:, rows + 3, where, :] = value

    def phi_copies(section):
        slot = 2 * section
        return [
            remote(
                edge.at[slot + side], halo.at[slot + side],
                phi_send.at[section], phi_recv.at[section], phi_peer(jump),
            )
            for side, jump in ((0, wedges - 1), (1, 1))
        ]

    def phi_both(section):
        slots = pl.ds(2 * section, 2)
        return remote(
            edge.at[slots], halo.at[slots], phi_send.at[section], phi_recv.at[section],
            phi_peer(1),
        )

    def phi_pack(buffer, section):
        for side, start in ((0, PAD), (1, PAD + cells - 2)):
            edge[section * 2 + side] = buffer[:, pl.ds(2, rows), pl.ds(start, 2), :]

    def phi_unpack(buffer, section):
        for side, start in ((0, PAD + cells), (1, PAD - 2)):
            buffer[:, pl.ds(2, rows), pl.ds(start, 2), :] = halo[section * 2 + side]

    lane = lax.broadcasted_iota(jnp.int32, (rows, lanes), 1)
    line = lax.broadcasted_iota(jnp.int32, (rows, lanes), 0)
    column = jnp.sum(first[0, pl.ds(2, rows), pl.ds(PAD, cells), :], axis=1)
    column = jnp.sum(column * table[0:1, :], axis=1, keepdims=True)
    centres = INNER_RADIUS + (
        (slab * rows + line).astype(jnp.float32) + 0.5
    ) * radial_step
    column = column * centres * centres * (radial_step * theta_step * phi_step)
    part[...] = jnp.sum(jnp.where(lane == line, column, 0.0), axis=0, keepdims=True)
    phi_pack(first, 0)

    sub = lax.broadcasted_iota(jnp.int32, shape, 0)
    lane_tile = lax.broadcasted_iota(jnp.int32, shape, 1)
    is_last = lane_tile == lanes - 1
    is_top, is_bottom = sub == TILE - 1, sub == 0

    def spread(value):
        return jnp.broadcast_to(value, shape)

    def radius_of(index):
        index = jnp.full(shape, slab * rows + index, jnp.int32).astype(jnp.float32)
        return INNER_RADIUS + (index + 0.5) * radial_step

    def radial_faces(buffer, low, count, tile):
        where = pl.ds(PAD + TILE * tile, TILE)
        lefts = [[] for _ in range(count)]
        rights = [[] for _ in range(count)]
        for k in range(variables):
            q = [buffer[k, low + j, where, :] for j in range(count + 3)]
            step = [q[j + 1] - q[j] for j in range(count + 2)]
            slope = [half_slope(step[j], step[j + 1]) for j in range(count + 1)]
            for i in range(count):
                lefts[i].append(q[i + 1] + slope[i])
                rights[i].append(q[i + 2] - slope[i + 1])
        out = []
        for i in range(count):
            face = radius_of(low + i) - 0.5 * radial_step
            out.append(flux(lefts[i], rights[i], 1, face * face * (0.5 / radial_step)))
        return out

    def radial_store(buffer, low, count):
        for t in range(tiles):
            for i, face in enumerate(radial_faces(buffer, low, count, t)):
                for k in range(variables):
                    radial[k, low + i, pl.ds(TILE * t, TILE), :] = face[k]

    def theta_part(centre):
        left, right = [], []
        for q in centre:
            after = pltpu.roll(q, lanes - 1, 1)
            above = jnp.where(is_last, 0.0, after - q)
            below = pltpu.roll(above, 1, 1)
            slope = half_slope(below, above)
            left.append(q + slope)
            right.append(pltpu.roll(q - slope, lanes - 1, 1))
        upper = flux(left, right, 2, spread(table[1:2, :]))
        return [pltpu.roll(f, 1, 1) - f for f in upper]

    def phi_ends(buffer):
        def column_at(k, cell):
            return buffer[k, pl.ds(2, rows), PAD + cell, :]

        left, right = [], []
        for k in range(variables):
            a, b, c, d = (column_at(k, cell) for cell in (-2, -1, 0, 1))
            left.append(b + half_slope(b - a, c - b))
            right.append(c - half_slope(c - b, d - c))
            a, b, c = (column_at(k, cell) for cell in (cells - 1, cells, cells + 1))
            ends[1, k] = b - half_slope(b - a, c - b)
        for k, f in enumerate(flux(left, right, 3, 0.5 / phi_step)):
            ends[0, k] = f

    def phi_part(buffer, r):
        left, right = [[] for _ in range(tiles)], [[] for _ in range(tiles)]
        for k in range(variables):
            turned = []
            for t in range(tiles):
                start = PAD + TILE * t
                a, b, c = (
                    buffer[k, r + 2, pl.ds(start + offset, TILE), :] for offset in (-1, 0, 1)
                )
                slope = half_slope(b - a, c - b)
                left[t].append(b + slope)
                turned.append(pltpu.roll(b - slope, TILE - 1, 0))
            turned.append(spread(ends[1, k, pl.ds(r, 1), :]))
            for t in range(tiles):
                right[t].append(jnp.where(is_top, turned[t + 1], turned[t]))
        upper = [flux(left[t], right[t], 3, 0.5 / phi_step) for t in range(tiles)]
        out = [[] for _ in range(tiles)]
        for k in range(variables):
            before = spread(ends[0, k, pl.ds(r, 1), :])
            for t in range(tiles):
                turned = pltpu.roll(upper[t][k], 1, 0)
                out[t].append(jnp.where(is_bottom, before, turned) - upper[t][k])
                before = turned
        return out

    def sources(centre, inverse_r):
        density, inverse, pressure = thermo(centre)
        vr, vt, vp = (centre[m] * inverse for m in (1, 2, 3))
        cot = spread(table[2:3, :])
        swirl = density * vp * vp
        return density, [
            (2.0 * pressure + density * vt * vt + swirl) * inverse_r,
            ((pressure + swirl) * cot - density * vr * vt) * inverse_r,
            -density * vp * (vr + vt * cot) * inverse_r,
        ]

    def centre_at(buffer, r, tile):
        return [
            buffer[k, r + 2, pl.ds(PAD + TILE * tile, TILE), :] for k in range(variables)
        ]

    def early_one(r):
        inverse_r = 1.0 / radius_of(r)
        around = inverse_r * spread(table[3:4, :]) * timestep
        for t in range(tiles):
            centre = centre_at(first, r, t)
            total = [c + d * around for c, d in zip(centre, theta_part(centre))]
            _, source = sources(centre, inverse_r)
            for m in range(3):
                total[m + 1] = total[m + 1] + timestep * source[m]
            for k in range(variables):
                second[k, r + 2, pl.ds(PAD + TILE * t, TILE), :] = total[k]

    def late_one(r):
        inverse_r = 1.0 / radius_of(r)
        around = inverse_r * spread(table[3:4, :]) * timestep
        along = inverse_r * inverse_r * timestep
        for t, part_of in enumerate(phi_part(first, r)):
            into = pl.ds(TILE * t, TILE)
            where = pl.ds(PAD + TILE * t, TILE)
            for k in range(variables):
                across = radial[k, r, into, :] - radial[k, r + 1, into, :]
                second[k, r + 2, where, :] = (
                    second[k, r + 2, where, :] + part_of[k] * around + across * along
                )

    def section_two(r):
        inverse_r = 1.0 / radius_of(r)
        scale = 0.5 * timestep
        around = inverse_r * spread(table[3:4, :]) * scale
        along = inverse_r * inverse_r * scale
        gravity = spread(pull[pl.ds(r + 8, 1), :])
        phi = phi_part(second, r)
        for t in range(tiles):
            into = pl.ds(TILE * t, TILE)
            where = pl.ds(PAD + TILE * t, TILE)
            upper = radial_faces(second, r + 1, 1, t)[0]
            lower = [radial[k, r, into, :] for k in range(variables)]
            for k in range(variables):
                radial[k, r + 1, into, :] = upper[k]
            centre = centre_at(second, r, t)
            theta = theta_part(centre)
            density, source = sources(centre, inverse_r)
            source[0] = source[0] - density * gravity
            source.append(-centre[1] * gravity)
            total = [
                0.5 * (first[k, r + 2, where, :] + centre[k])
                + (theta[k] + phi[t][k]) * around
                + (lower[k] - upper[k]) * along
                for k in range(variables)
            ]
            for m in range(4):
                total[m + 1] = total[m + 1] + scale * source[m]
            for k in range(variables):
                out_ref[k, r, into, :] = total[k]

    def each_pair(low, high, step):
        def both(i):
            step(2 * i)
            step(2 * i + 1)

        each(low // 2, high // 2, both)

    pl.semaphore_wait(barrier, greeted)

    def reply(v):
        pl.when(v < slab)(lambda: signal(far.at[jnp.where(z < TOP, 0, 1)], (v, wedge)))

    part_copies = [
        remote(part, got_part.at[j], part_send.at[0], part_recv.at[0], phi_peer(j))
        for j in range(1, wedges)
    ]
    others = pl.ds(1, wedges - 1)
    part_all = remote(
        got_part.at[others], got_part.at[others], part_send.at[0], part_recv.at[0], phi_peer(1)
    )
    first_radial, second_radial = radial_copies(first, 0), radial_copies(second, 1)
    first_phi, second_phi = phi_copies(0), phi_copies(1)
    for copy in part_copies:
        copy.start()
    radial_start(first_radial)
    for copy in first_phi:
        copy.start()

    pl.when(slab % LINE == LINE - 2)(lambda: signal(told, (slab + 1, wedge)))

    @pl.when(jnp.logical_not(turned_last))
    def _():
        each_slab(0, level, reply)

    got_part[0] = part[...]
    each_pair(0, rows, early_one)
    each(0, 2, lambda i: radial_store(first, 2 + 2 * i, 2))
    radial_store(first, 6, 1)

    @pl.when(turned_last)
    def _():
        pl.semaphore_wait(told, 1)
        each_slab(0, level, reply)

    part_all.wait_recv()
    shells = jnp.zeros((1, lanes), jnp.float32)
    for w in range(wedges):
        shells = shells + got_part[lax.rem(wedge + wedges - w, wedges)]
    slab_part[...] = shells

    def slab_copy(source, target):
        return remote(
            slab_part, got.at[source], slab_send.at[0], slab_recv.at[0], (target, wedge),
        )

    def slab_all(count):
        ref = got.at[pl.ds(0, count)]
        return remote(ref, ref, slab_send.at[0], slab_recv.at[0], radial_peer(0))

    def by_slab(low, high, step):
        if high - low == 1:
            step(low)
            return
        middle = (low + high) // 2
        pl.when(slab < middle)(lambda: by_slab(low, middle, step))
        pl.when(slab >= middle)(lambda: by_slab(middle, high, step))

    def slab_start(v):
        pl.when(v > slab)(lambda: slab_copy(slab, v).start())

    above_copy = remote(
        slab_part, got_above, slab_send.at[0], above_recv.at[0], radial_peer(-1)
    )
    each_slab(0, level + 1, slab_start)
    pl.when(has_down)(above_copy.start)

    def send_out():
        for at, low, high in ((0, level + 1, TOP), (1, jnp.maximum(level + 1, TOP), levels)):
            @pl.when(heard[at] > 0)
            def _():
                pl.semaphore_wait(far.at[at], heard[at])
                each_slab(low, high, slab_start)

    phi_both(0).wait_recv()
    phi_unpack(first, 0)
    pl.when(turns)(send_out)
    radial_land(first_radial)
    radial_ends(first)
    phi_ends(first)
    each(0, 2, lambda i: radial_store(first, 7 * i, 2))
    each(0, 4, lambda i: late_one(i + (i // 2) * (rows - 4)))
    radial_sent(first_radial)
    radial_start(second_radial)
    each(2, rows - 2, late_one)
    phi_pack(second, 1)
    for copy in second_phi:
        copy.start()

    pl.when(jnp.logical_not(turns))(send_out)

    after = jnp.where(lane < line, 1.0, jnp.where(lane == line, 0.5, 0.0))
    within = jnp.sum(after * slab_part[...], axis=1, keepdims=True)
    whole = jnp.sum(jnp.where(line >= 0, slab_part[...], 0.0), axis=1, keepdims=True)

    phi_both(1).wait_recv()
    phi_unpack(second, 1)
    radial_land(second_radial)

    part_all.wait_send()
    phi_both(0).wait_send()
    phi_both(1).wait_send()
    radial_sent(second_radial)
    by_slab(0, slabs, lambda s: slab_all(slabs - max(s, 1)).wait_send())
    pl.when(has_up)(above_copy.wait_recv)
    by_slab(0, slabs, lambda s: slab_all(s).wait_recv() if s else None)
    sums = [jnp.zeros((1, lanes), jnp.float32) for _ in range(4)]
    for v in range(slabs - 1):
        sums[v % 4] = sums[v % 4] + jnp.where(slab > v, got[v], 0.0)
    before = jnp.broadcast_to((sums[0] + sums[1]) + (sums[2] + sums[3]), (rows, lanes))
    before = core[0] + jnp.sum(before, axis=1, keepdims=True)
    inner = jnp.where(lane > line, 1.0, jnp.where(lane == line, 0.5, 0.0))
    inner = jnp.sum(inner * got[jnp.maximum(slab - 1, 0)], axis=1, keepdims=True)
    outer = jnp.sum(after * got_above[...], axis=1, keepdims=True)
    wide = jnp.zeros((rows, lanes), jnp.float32)
    enclosed = before + within + wide
    mass_ref[...] = jnp.sum(jnp.where(lane == line, enclosed, 0.0), axis=0, keepdims=True)[:, :rows]
    for i, inside in ((0, before - inner), (1, before + within), (2, before + whole + outer)):
        at = centres + (i - 1) * rows * radial_step
        pull[pl.ds(8 * i, 8), :] = strength * (inside + wide) / (at * at)

    def pulled(row, start):
        where = pl.ds(start, TILE)
        gravity = timestep * spread(pull[pl.ds(row + 6, 1), :])
        density = jnp.maximum(first[0, row, where, :], MINIMUM_DENSITY)
        second[1, row, where, :] = second[1, row, where, :] - density * gravity
        second[4, row, where, :] = second[4, row, where, :] - first[1, row, where, :] * gravity

    def pulled_row(row):
        for t in range(-1, tiles + 1):
            pulled(row, PAD + TILE * t)

    each_pair(0, rows + 4, pulled_row)
    radial_ends(second)

    phi_ends(second)
    radial_store(second, 0, 1)
    each_pair(0, rows, section_two)


def body(conserved, core_mass):
    variables, rows, cells, lanes = conserved.shape
    slabs, wedges = lax.axis_size("radial"), lax.axis_size("phi")
    sizes = step_sizes(rows * slabs, cells * wedges, lanes)
    table = jnp.asarray(angle_tables(lanes, sizes[1]))
    padded = (variables, rows + 4, cells + 2 * PAD, lanes)
    vmem = pl.BlockSpec(memory_space=pltpu.VMEM)
    dma = pltpu.SemaphoreType.DMA
    advanced, mass = pl.pallas_call(
        functools.partial(kernel, sizes, (slabs, wedges)),
        out_shape=(
            pltpu.VMEM(conserved.shape, jnp.float32),
            pltpu.VMEM((1, rows), jnp.float32),
        ),
        in_specs=[pl.BlockSpec(memory_space=pl.ANY)] * 3,
        out_specs=(vmem, vmem),
        scratch_shapes=[
            pltpu.VMEM(padded, jnp.float32),
            pltpu.VMEM(padded, jnp.float32),
            pltpu.VMEM((4, variables, rows, 2, lanes), jnp.float32),
            pltpu.VMEM((4, variables, rows, 2, lanes), jnp.float32),
            pltpu.VMEM((variables, rows + 1, cells, lanes), jnp.float32),
            pltpu.VMEM((2, variables, rows, lanes), jnp.float32),
            pltpu.VMEM((1, lanes), jnp.float32),
            pltpu.VMEM((1, lanes), jnp.float32),
            pltpu.VMEM((wedges, 1, lanes), jnp.float32),
            pltpu.VMEM((slabs, 1, lanes), jnp.float32),
            pltpu.VMEM((1, lanes), jnp.float32),
            pltpu.VMEM((3 * TILE, lanes), jnp.float32),
            pltpu.VMEM((TILE, lanes), jnp.float32),
            pltpu.SMEM((1,), jnp.float32),
            pltpu.SemaphoreType.REGULAR((2,)),
            pltpu.SemaphoreType.REGULAR,
            dma((3,)),
            dma((2,)),
            dma((4,)),
            dma((2,)),
            dma((2,)),
            dma((1,)),
            dma((1,)),
            dma((1,)),
            dma((1,)),
            dma((1,)),
        ],
        compiler_params=pltpu.CompilerParams(collective_id=0, has_side_effects=True),
    )(core_mass, table, conserved)
    return advanced, mass.reshape(rows)


def solution(mesh):
    in_specs = (P(None, "radial", "phi", None), P())
    out_specs = (P(None, "radial", "phi", None), P("radial"))
    return jax.shard_map(body, mesh=mesh, in_specs=in_specs, out_specs=out_specs, check_vma=False)
```

```python
import functools
import math
import types

import jax
import jax.numpy as jnp
import numpy as np
from jax import lax
from jax.experimental import pallas as pl
from jax.experimental.pallas import tpu as pltpu
from jax.sharding import PartitionSpec as P

ADIABATIC = 4.0 / 3.0
INNER_RADIUS = 1.0
OUTER_RADIUS = 2.0
COURANT = 0.4
GRAVITY_KICK = 0.004
MINIMUM_DENSITY = 0.05
PRESSURE_FLOOR = 0.01
MESH = pl.DeviceIdType.MESH
TILE = 8
PAD = 8
DEPTH = 8
LINE = 2 * DEPTH
TOP = 4


def step_sizes(radial_total, phi_total, theta_total):
    theta_step = math.pi / theta_total
    phi_step = 2.0 * math.pi / phi_total
    polar_width = INNER_RADIUS * math.sin(0.5 * theta_step) * phi_step
    radial_step = min(2.0 * polar_width, (OUTER_RADIUS - INNER_RADIUS) / radial_total)
    timestep = COURANT * min(radial_step, polar_width)
    return (radial_step, theta_step, phi_step, timestep)


def angle_tables(theta_cells, theta_step):
    step = np.float32(theta_step)
    centre = (np.arange(theta_cells, dtype=np.float32) + np.float32(0.5)) * step
    face = np.arange(theta_cells + 1, dtype=np.float32) * step
    sine = np.sin(centre.astype(np.float64))
    cosine = np.cos(centre.astype(np.float64))
    face_sine = np.sin(face.astype(np.float64))
    face_sine[-1] = 0.0
    zero = np.zeros(theta_cells)
    upper = 0.5 * face_sine[1:] / theta_step
    rows = [sine, upper, cosine / sine, 1.0 / sine, zero, zero, zero, zero]
    return np.stack(rows).astype(np.float32)


def half_slope(below, above):
    high, low = jnp.maximum(below, 0.0), jnp.minimum(below, 0.0)
    return 0.5 * jnp.maximum(jnp.minimum(above, high), low)


def thermo(q):
    density = jnp.maximum(q[0], MINIMUM_DENSITY)
    inverse = 1.0 / density
    kinetic = 0.5 * (q[1] * q[1] + q[2] * q[2] + q[3] * q[3]) * inverse
    pressure = jnp.maximum((ADIABATIC - 1.0) * (q[4] - kinetic), PRESSURE_FLOOR * density)
    return density, inverse, pressure


def physical(q, component):
    _, inverse, pressure = thermo(q)
    normal = q[component] * inverse
    squared = ADIABATIC * pressure * inverse
    return normal, pressure, jnp.abs(normal) + squared * lax.rsqrt(squared)


def flux(left, right, component, half_area):
    left_v, left_p, left_a = physical(left, component)
    right_v, right_p, right_a = physical(right, component)
    signal = jnp.maximum(left_a, right_a)
    left_w = half_area * (left_v + signal)
    right_w = half_area * (right_v - signal)
    out = [a * left_w + b * right_w for a, b in zip(left, right)]
    out[component] = out[component] + half_area * (left_p + right_p)
    out[4] = out[4] + half_area * (left_p * left_v + right_p * right_v)
    return out


def each(low, high, step):
    lax.fori_loop(low, high, lambda r, _: (step(r), 0)[1], 0)


def each_pair(low, high, step):
    def both(i):
        step(2 * i)
        step(2 * i + 1)

    each(low // 2, high // 2, both)


def stencils(sizes, extent, slab, table, ends, radial):
    radial_step, theta_step, phi_step, _ = sizes
    variables, rows, cells, lanes = extent
    tiles = cells // TILE
    shape = (TILE, lanes)
    sub = lax.broadcasted_iota(jnp.int32, shape, 0)
    lane_tile = lax.broadcasted_iota(jnp.int32, shape, 1)
    is_last = lane_tile == lanes - 1
    is_top, is_bottom = sub == TILE - 1, sub == 0

    def spread(value):
        return jnp.broadcast_to(value, shape)

    def radius_of(index):
        index = jnp.full(shape, slab * rows + index, jnp.int32).astype(jnp.float32)
        return INNER_RADIUS + (index + 0.5) * radial_step

    def radial_faces(buffer, low, count, tile):
        where = pl.ds(PAD + TILE * tile, TILE)
        lefts = [[] for _ in range(count)]
        rights = [[] for _ in range(count)]
        for k in range(variables):
            q = [buffer[k, low + j, where, :] for j in range(count + 3)]
            step = [q[j + 1] - q[j] for j in range(count + 2)]
            slope = [half_slope(step[j], step[j + 1]) for j in range(count + 1)]
            for i in range(count):
                lefts[i].append(q[i + 1] + slope[i])
                rights[i].append(q[i + 2] - slope[i + 1])
        out = []
        for i in range(count):
            face = radius_of(low + i) - 0.5 * radial_step
            out.append(flux(lefts[i], rights[i], 1, face * face * (0.5 / radial_step)))
        return out

    def radial_store(buffer, low, count):
        for t in range(tiles):
            for i, face in enumerate(radial_faces(buffer, low, count, t)):
                for k in range(variables):
                    radial[k, low + i, pl.ds(TILE * t, TILE), :] = face[k]

    def theta_part(centre):
        left, right = [], []
        for q in centre:
            after = pltpu.roll(q, lanes - 1, 1)
            above = jnp.where(is_last, 0.0, after - q)
            below = pltpu.roll(above, 1, 1)
            slope = half_slope(below, above)
            left.append(q + slope)
            right.append(pltpu.roll(q - slope, lanes - 1, 1))
        upper = flux(left, right, 2, spread(table[1:2, :]))
        return [pltpu.roll(f, 1, 1) - f for f in upper]

    def phi_ends(buffer):
        def column_at(k, cell):
            return buffer[k, pl.ds(2, rows), PAD + cell, :]

        left, right = [], []
        for k in range(variables):
            a, b, c, d = (column_at(k, cell) for cell in (-2, -1, 0, 1))
            left.append(b + half_slope(b - a, c - b))
            right.append(c - half_slope(c - b, d - c))
            a, b, c = (column_at(k, cell) for cell in (cells - 1, cells, cells + 1))
            ends[1, k] = b - half_slope(b - a, c - b)
        for k, f in enumerate(flux(left, right, 3, 0.5 / phi_step)):
            ends[0, k] = f

    def phi_part(buffer, r):
        left, right = [[] for _ in range(tiles)], [[] for _ in range(tiles)]
        for k in range(variables):
            turned = []
            for t in range(tiles):
                start = PAD + TILE * t
                a, b, c = (
                    buffer[k, r + 2, pl.ds(start + offset, TILE), :] for offset in (-1, 0, 1)
                )
                slope = half_slope(b - a, c - b)
                left[t].append(b + slope)
                turned.append(pltpu.roll(b - slope, TILE - 1, 0))
            turned.append(spread(ends[1, k, pl.ds(r, 1), :]))
            for t in range(tiles):
                right[t].append(jnp.where(is_top, turned[t + 1], turned[t]))
        upper = [flux(left[t], right[t], 3, 0.5 / phi_step) for t in range(tiles)]
        out = [[] for _ in range(tiles)]
        for k in range(variables):
            before = spread(ends[0, k, pl.ds(r, 1), :])
            for t in range(tiles):
                turned = pltpu.roll(upper[t][k], 1, 0)
                out[t].append(jnp.where(is_bottom, before, turned) - upper[t][k])
                before = turned
        return out

    def sources(centre, inverse_r):
        density, inverse, pressure = thermo(centre)
        vr, vt, vp = (centre[m] * inverse for m in (1, 2, 3))
        cot = spread(table[2:3, :])
        swirl = density * vp * vp
        return density, [
            (2.0 * pressure + density * vt * vt + swirl) * inverse_r,
            ((pressure + swirl) * cot - density * vr * vt) * inverse_r,
            -density * vp * (vr + vt * cot) * inverse_r,
        ]

    def centre_at(buffer, r, tile):
        return [
            buffer[k, r + 2, pl.ds(PAD + TILE * tile, TILE), :] for k in range(variables)
        ]

    return types.SimpleNamespace(
        spread=spread,
        radius_of=radius_of,
        radial_faces=radial_faces,
        radial_store=radial_store,
        theta_part=theta_part,
        phi_ends=phi_ends,
        phi_part=phi_part,
        sources=sources,
        centre_at=centre_at,
    )


def kernel(
    sizes,
    counts,
    core_ref,
    table_ref,
    input_ref,
    first,
    second,
    pull,
    table,
    mass_ref,
    edge,
    halo,
    radial,
    ends,
    part,
    slab_part,
    got_part,
    got,
    got_above,
    core,
    far,
    told,
    load_sem,
    radial_send,
    radial_recv,
    phi_send,
    phi_recv,
    part_send,
    part_recv,
    slab_send,
    slab_recv,
    above_recv,
):
    radial_step, theta_step, phi_step, timestep = sizes
    slabs, wedges = counts
    variables, rows, cells, lanes = input_ref.shape
    tiles = cells // TILE
    strength = GRAVITY_KICK / timestep
    slab, wedge = lax.axis_index("radial"), lax.axis_index("phi")
    has_up, has_down = slab < slabs - 1, slab > 0
    shape = (TILE, lanes)

    load = pltpu.make_async_copy(
        input_ref, first.at[:, pl.ds(2, rows), pl.ds(PAD, cells), :], load_sem.at[0]
    )
    load.start()
    load_table = pltpu.make_async_copy(table_ref, table, load_sem.at[1])
    load_table.start()
    load_core = pltpu.make_async_copy(core_ref, core, load_sem.at[2])
    load_core.start()

    def radial_peer(jump):
        return (slab + jump, wedge)

    def phi_peer(jump):
        return (slab, lax.rem(wedge + jump, wedges))

    barrier = pltpu.get_barrier_semaphore()
    x, z, c = slab // LINE, (slab // 2) % DEPTH, slab % 2
    level = jnp.where(z < TOP, z, TOP + x)
    rank = jnp.where(z < TOP, 2 * x + c, 2 * (z - TOP) + c)
    span, levels = slabs // DEPTH, DEPTH
    turns = jnp.logical_and(slab % LINE == 0, has_down)
    turned_last = slab % LINE == LINE - 1
    turned_to = jnp.logical_and(turned_last, has_up)

    def signal(semaphore, peer):
        pl.semaphore_signal(semaphore, inc=1, device_id=peer, device_id_type=MESH)

    def each_slab(low, high, step):
        def one_level(at):
            for i in range(span):
                spread_out = LINE * (i // 2) + 2 * at + i % 2
                step(jnp.where(at < TOP, spread_out, LINE * (at - TOP) + LINE // 2 + i))

        each(low, high, one_level)

    def greet(v):
        signal(barrier, (v, wedge))

    def greet_level(v):
        pl.when(jnp.logical_or(v < slab, v == slab + 1))(lambda: greet(v))

    def greet_outer(v):
        known = jnp.logical_or(v % LINE != LINE - 1, v == slab - 1)
        pl.when(known)(lambda: greet(v))

    for j in range(1, wedges):
        signal(barrier, phi_peer(j))
    pl.when(jnp.logical_and(z > 0, jnp.logical_and(z <= TOP, c == 0)))(lambda: greet(slab - 1))
    pl.when(turned_to)(lambda: greet(slab + 1))
    each_slab(level, level + 1, greet_level)
    each_slab(level + 1, levels, greet_outer)
    inside = jnp.where(z < TOP, 2 * c, jnp.where(rank > 0, 1, 0))
    inside = jnp.where(turned_last, jnp.where(has_up, 2, 1), span * level + span - 1 - rank + inside)
    greeted = (wedges - 1) + inside + jnp.where(turns, 1, 0)
    further = slabs // LINE - 1 - x
    heard = (
        jnp.where(z < TOP, (TOP - 1 - z) * 2 * (further + 1), 0),
        jnp.where(z < TOP, (DEPTH - TOP) * 2 * (further + 1), span * further),
    )

    load.wait()
    load_table.wait()
    load_core.wait()

    def remote(src, dst, send, recv, peer):
        return pltpu.make_async_remote_copy(
            src_ref=src, dst_ref=dst, send_sem=send, recv_sem=recv, device_id=peer,
            device_id_type=MESH,
        )

    def radial_copies(buffer, section):
        where, slot = pl.ds(PAD, cells), 2 * section
        up = remote(
            buffer.at[:, pl.ds(rows, 2), where, :], buffer.at[:, pl.ds(0, 2), where, :],
            radial_send.at[0], radial_recv.at[slot], radial_peer(1),
        )
        down = remote(
            buffer.at[:, pl.ds(2, 2), where, :], buffer.at[:, pl.ds(rows + 2, 2), where, :],
            radial_send.at[1], radial_recv.at[slot + 1], radial_peer(-1),
        )
        return up, down

    def radial_start(copies):
        up, down = copies
        pl.when(has_up)(up.start)
        pl.when(has_down)(down.start)

    def radial_sent(copies):
        up, down = copies
        pl.when(has_up)(up.wait_send)
        pl.when(has_down)(down.wait_send)

    def radial_land(copies):
        up, down = copies
        pl.when(has_down)(up.wait_recv)
        pl.when(has_up)(down.wait_recv)

    def radial_ends(buffer):
        for t in range(tiles):
            where = pl.ds(PAD + TILE * t, TILE)

            @pl.when(jnp.logical_not(has_down))
            def _():
                value = buffer[:, 2, where, :]
                buffer[:, 0, where, :] = value
                buffer[:, 1, where, :] = value

            @pl.when(jnp.logical_not(has_up))
            def _():
                value = buffer[:, rows + 1, where, :]
                buffer[:, rows + 2, where, :] = value
                buffer[:, rows + 3, where, :] = value

    whole, inside_rows, edge_rows = [(0, rows)], [(2, rows - 4)], [(0, 2), (rows - 2, 2)]

    def phi_copies(section, count):
        slot = 2 * section
        return [
            remote(
                edge.at[slot + side, :, pl.ds(0, count)],
                halo.at[slot + side, :, pl.ds(0, count)],
                phi_send.at[section], phi_recv.at[section], phi_peer(jump),
            )
            for side, jump in ((0, wedges - 1), (1, 1))
        ]

    def phi_both(section, count):
        where = (pl.ds(2 * section, 2), slice(None), pl.ds(0, count))
        return remote(
            edge.at[where], halo.at[where], phi_send.at[section], phi_recv.at[section],
            phi_peer(1),
        )

    def phi_pack(buffer, section, pieces):
        for side, start in ((0, PAD), (1, PAD + cells - 2)):
            at = 0
            for begin, count in pieces:
                edge[section * 2 + side, :, pl.ds(at, count)] = buffer[
                    :, pl.ds(2 + begin, count), pl.ds(start, 2), :
                ]
                at += count

    def phi_unpack(buffer, section, pieces):
        for side, start in ((0, PAD + cells), (1, PAD - 2)):
            at = 0
            for begin, count in pieces:
                buffer[:, pl.ds(2 + begin, count), pl.ds(start, 2), :] = halo[
                    section * 2 + side, :, pl.ds(at, count)
                ]
                at += count

    lane = lax.broadcasted_iota(jnp.int32, (rows, lanes), 1)
    line = lax.broadcasted_iota(jnp.int32, (rows, lanes), 0)
    column = jnp.sum(first[0, pl.ds(2, rows), pl.ds(PAD, cells), :], axis=1)
    column = jnp.sum(column * table[0:1, :], axis=1, keepdims=True)
    centres = INNER_RADIUS + (
        (slab * rows + line).astype(jnp.float32) + 0.5
    ) * radial_step
    column = column * centres * centres * (radial_step * theta_step * phi_step)
    part[...] = jnp.sum(jnp.where(lane == line, column, 0.0), axis=0, keepdims=True)
    phi_pack(first, 0, whole)

    on = stencils(sizes, input_ref.shape, slab, table, ends, radial)

    def early_one(r):
        inverse_r = 1.0 / on.radius_of(r)
        around = inverse_r * on.spread(table[3:4, :]) * timestep
        for t in range(tiles):
            centre = on.centre_at(first, r, t)
            total = [c + d * around for c, d in zip(centre, on.theta_part(centre))]
            _, source = on.sources(centre, inverse_r)
            for m in range(3):
                total[m + 1] = total[m + 1] + timestep * source[m]
            for k in range(variables):
                second[k, r + 2, pl.ds(PAD + TILE * t, TILE), :] = total[k]

    def late_one(r):
        inverse_r = 1.0 / on.radius_of(r)
        around = inverse_r * on.spread(table[3:4, :]) * timestep
        along = inverse_r * inverse_r * timestep
        for t, part_of in enumerate(on.phi_part(first, r)):
            into = pl.ds(TILE * t, TILE)
            where = pl.ds(PAD + TILE * t, TILE)
            for k in range(variables):
                across = radial[k, r, into, :] - radial[k, r + 1, into, :]
                second[k, r + 2, where, :] = (
                    second[k, r + 2, where, :] + part_of[k] * around + across * along
                )

    pl.semaphore_wait(barrier, greeted)

    def reply(v):
        pl.when(v < slab)(lambda: signal(far.at[jnp.where(z < TOP, 0, 1)], (v, wedge)))

    part_copies = [
        remote(part, got_part.at[j], part_send.at[0], part_recv.at[0], phi_peer(j))
        for j in range(1, wedges)
    ]
    others = pl.ds(1, wedges - 1)
    part_all = remote(
        got_part.at[others], got_part.at[others], part_send.at[0], part_recv.at[0], phi_peer(1)
    )
    first_radial, second_radial = radial_copies(first, 0), radial_copies(second, 1)
    first_phi = phi_copies(0, rows)
    inside_phi, edge_phi = phi_copies(1, rows - 4), phi_copies(2, 4)
    for copy in part_copies:
        copy.start()
    radial_start(first_radial)
    for copy in first_phi:
        copy.start()

    pl.when(slab % LINE == LINE - 2)(lambda: signal(told, (slab + 1, wedge)))

    @pl.when(jnp.logical_not(turned_last))
    def _():
        each_slab(0, level, reply)

    got_part[0] = part[...]
    each_pair(0, rows, early_one)
    each(0, 2, lambda i: on.radial_store(first, 2 + 2 * i, 2))
    on.radial_store(first, 6, 1)

    @pl.when(turned_last)
    def _():
        pl.semaphore_wait(told, 1)
        each_slab(0, level, reply)

    part_all.wait_recv()
    shells = jnp.zeros((1, lanes), jnp.float32)
    for w in range(wedges):
        shells = shells + got_part[lax.rem(wedge + wedges - w, wedges)]
    slab_part[...] = shells

    def slab_copy(source, target):
        return remote(
            slab_part, got.at[source], slab_send.at[0], slab_recv.at[0], (target, wedge),
        )

    def slab_all(count):
        ref = got.at[pl.ds(0, count)]
        return remote(ref, ref, slab_send.at[0], slab_recv.at[0], radial_peer(0))

    def by_slab(low, high, step):
        if high - low == 1:
            step(low)
            return
        middle = (low + high) // 2
        pl.when(slab < middle)(lambda: by_slab(low, middle, step))
        pl.when(slab >= middle)(lambda: by_slab(middle, high, step))

    def slab_start(v):
        pl.when(v > slab)(lambda: slab_copy(slab, v).start())

    above_copy = remote(
        slab_part, got_above, slab_send.at[0], above_recv.at[0], radial_peer(-1)
    )
    each_slab(0, level + 1, slab_start)
    pl.when(has_down)(above_copy.start)

    def send_out():
        for at, low, high in ((0, level + 1, TOP), (1, jnp.maximum(level + 1, TOP), levels)):
            @pl.when(heard[at] > 0)
            def _():
                pl.semaphore_wait(far.at[at], heard[at])
                each_slab(low, high, slab_start)

    phi_both(0, rows).wait_recv()
    phi_unpack(first, 0, whole)
    on.phi_ends(first)
    each(2, rows - 2, late_one)
    phi_pack(second, 1, inside_rows)
    for copy in inside_phi:
        copy.start()
    pl.when(turns)(send_out)
    radial_land(first_radial)
    radial_ends(first)
    each(0, 2, lambda i: on.radial_store(first, 7 * i, 2))
    each(0, 4, lambda i: late_one(i + (i // 2) * (rows - 4)))
    radial_sent(first_radial)
    radial_start(second_radial)
    phi_pack(second, 2, edge_rows)
    for copy in edge_phi:
        copy.start()
    pl.when(jnp.logical_not(turns))(send_out)

    after = jnp.where(lane < line, 1.0, jnp.where(lane == line, 0.5, 0.0))
    within = jnp.sum(after * slab_part[...], axis=1, keepdims=True)
    whole = jnp.sum(jnp.where(line >= 0, slab_part[...], 0.0), axis=1, keepdims=True)

    phi_both(1, rows - 4).wait_recv()
    phi_unpack(second, 1, inside_rows)
    phi_both(2, 4).wait_recv()
    phi_unpack(second, 2, edge_rows)
    radial_land(second_radial)

    part_all.wait_send()
    phi_both(0, rows).wait_send()
    phi_both(1, rows - 4).wait_send()
    phi_both(2, 4).wait_send()
    radial_sent(second_radial)
    by_slab(0, slabs, lambda s: slab_all(slabs - max(s, 1)).wait_send())
    pl.when(has_up)(above_copy.wait_recv)
    by_slab(0, slabs, lambda s: slab_all(s).wait_recv() if s else None)
    sums = [jnp.zeros((1, lanes), jnp.float32) for _ in range(4)]
    for v in range(slabs - 1):
        sums[v % 4] = sums[v % 4] + jnp.where(slab > v, got[v], 0.0)
    before = jnp.broadcast_to((sums[0] + sums[1]) + (sums[2] + sums[3]), (rows, lanes))
    before = core[0] + jnp.sum(before, axis=1, keepdims=True)
    inner = jnp.where(lane > line, 1.0, jnp.where(lane == line, 0.5, 0.0))
    inner = jnp.sum(inner * got[jnp.maximum(slab - 1, 0)], axis=1, keepdims=True)
    outer = jnp.sum(after * got_above[...], axis=1, keepdims=True)
    wide = jnp.zeros((rows, lanes), jnp.float32)
    enclosed = before + within + wide
    mass_ref[...] = jnp.sum(jnp.where(lane == line, enclosed, 0.0), axis=0, keepdims=True)[:, :rows]
    for i, inside in ((0, before - inner), (1, before + within), (2, before + whole + outer)):
        at = centres + (i - 1) * rows * radial_step
        pull[pl.ds(8 * i, 8), :] = strength * (inside + wide) / (at * at)

    def pulled(row, start):
        where = pl.ds(start, TILE)
        gravity = timestep * on.spread(pull[pl.ds(row + 6, 1), :])
        density = jnp.maximum(first[0, row, where, :], MINIMUM_DENSITY)
        second[1, row, where, :] = second[1, row, where, :] - density * gravity
        second[4, row, where, :] = second[4, row, where, :] - first[1, row, where, :] * gravity

    def pulled_row(row):
        for t in range(-1, tiles + 1):
            pulled(row, PAD + TILE * t)

    each_pair(0, rows + 4, pulled_row)
    radial_ends(second)


def finish(
    sizes,
    first,
    second,
    pull,
    table,
    mass,
    out_ref,
    mass_ref,
    out,
    ends,
    radial,
    sem,
):
    timestep = sizes[3]
    variables, rows, cells, lanes = out.shape
    tiles = cells // TILE
    slab = lax.axis_index("radial")
    on = stencils(sizes, out.shape, slab, table, ends, radial)
    save_mass = pltpu.make_async_copy(mass, mass_ref, sem.at[1])
    save_mass.start()

    def section_two(r):
        inverse_r = 1.0 / on.radius_of(r)
        scale = 0.5 * timestep
        around = inverse_r * on.spread(table[3:4, :]) * scale
        along = inverse_r * inverse_r * scale
        gravity = on.spread(pull[pl.ds(r + 8, 1), :])
        phi = on.phi_part(second, r)
        for t in range(tiles):
            into = pl.ds(TILE * t, TILE)
            where = pl.ds(PAD + TILE * t, TILE)
            centre = on.centre_at(second, r, t)
            theta = on.theta_part(centre)
            density, source = on.sources(centre, inverse_r)
            source[0] = source[0] - density * gravity
            source.append(-centre[1] * gravity)
            total = [
                0.5 * (first[k, r + 2, where, :] + centre[k])
                + (theta[k] + phi[t][k]) * around
                + (radial[k, r, into, :] - radial[k, r + 1, into, :]) * along
                for k in range(variables)
            ]
            for m in range(4):
                total[m + 1] = total[m + 1] + scale * source[m]
            for k in range(variables):
                out[k, r, into, :] = total[k]

    def save(i):
        where = (slice(None), pl.ds(2 * i, 2))
        return pltpu.make_async_copy(out.at[where], out_ref.at[where], sem.at[0])

    def two(i):
        section_two(2 * i)
        section_two(2 * i + 1)
        save(i).start()

    on.phi_ends(second)
    each(0, (rows + 1) // 3, lambda i: on.radial_store(second, 3 * i, 3))
    each(0, rows // 2, two)
    pltpu.make_async_copy(out, out_ref, sem.at[0]).wait()
    save_mass.wait()


def body(conserved, core_mass):
    variables, rows, cells, lanes = conserved.shape
    slabs, wedges = lax.axis_size("radial"), lax.axis_size("phi")
    sizes = step_sizes(rows * slabs, cells * wedges, lanes)
    table = jnp.asarray(angle_tables(lanes, sizes[1]))
    padded = (variables, rows + 4, cells + 2 * PAD, lanes)
    vmem = pl.BlockSpec(memory_space=pltpu.VMEM)
    dma = pltpu.SemaphoreType.DMA
    first, second, pull, table, mass = pl.pallas_call(
        functools.partial(kernel, sizes, (slabs, wedges)),
        out_shape=(
            pltpu.VMEM(padded, jnp.float32),
            pltpu.VMEM(padded, jnp.float32),
            pltpu.VMEM((3 * TILE, lanes), jnp.float32),
            pltpu.VMEM((TILE, lanes), jnp.float32),
            pltpu.VMEM((1, rows), jnp.float32),
        ),
        in_specs=[pl.BlockSpec(memory_space=pl.ANY)] * 3,
        out_specs=(vmem,) * 5,
        scratch_shapes=[
            pltpu.VMEM((6, variables, rows, 2, lanes), jnp.float32),
            pltpu.VMEM((6, variables, rows, 2, lanes), jnp.float32),
            pltpu.VMEM((variables, rows + 1, cells, lanes), jnp.float32),
            pltpu.VMEM((2, variables, rows, lanes), jnp.float32),
            pltpu.VMEM((1, lanes), jnp.float32),
            pltpu.VMEM((1, lanes), jnp.float32),
            pltpu.VMEM((wedges, 1, lanes), jnp.float32),
            pltpu.VMEM((slabs, 1, lanes), jnp.float32),
            pltpu.VMEM((1, lanes), jnp.float32),
            pltpu.SMEM((1,), jnp.float32),
            pltpu.SemaphoreType.REGULAR((2,)),
            pltpu.SemaphoreType.REGULAR,
            dma((3,)),
            dma((2,)),
            dma((4,)),
            dma((3,)),
            dma((3,)),
            dma((1,)),
            dma((1,)),
            dma((1,)),
            dma((1,)),
            dma((1,)),
        ],
        compiler_params=pltpu.CompilerParams(collective_id=0, has_side_effects=True),
    )(core_mass, table, conserved)
    advanced, mass = pl.pallas_call(
        functools.partial(finish, sizes),
        out_shape=(
            jax.ShapeDtypeStruct(conserved.shape, jnp.float32),
            jax.ShapeDtypeStruct((1, rows), jnp.float32),
        ),
        in_specs=[vmem] * 5,
        out_specs=(pl.BlockSpec(memory_space=pltpu.HBM),) * 2,
        scratch_shapes=[
            pltpu.VMEM(conserved.shape, jnp.float32),
            pltpu.VMEM((2, variables, rows, lanes), jnp.float32),
            pltpu.VMEM((variables, rows + 1, cells, lanes), jnp.float32),
            dma((2,)),
        ],
        compiler_params=pltpu.CompilerParams(vmem_limit_bytes=16 * 1024 * 1024),
    )(first, second, pull, table, mass)
    return advanced, mass.reshape(rows)


def solution(mesh):
    in_specs = (P(None, "radial", "phi", None), P())
    out_specs = (P(None, "radial", "phi", None), P("radial"))
    return jax.shard_map(body, mesh=mesh, in_specs=in_specs, out_specs=out_specs, check_vma=False)
```

```python
import functools
import math
import types

import jax
import jax.numpy as jnp
import numpy as np
from jax import lax
from jax.experimental import pallas as pl
from jax.experimental.pallas import tpu as pltpu
from jax.sharding import PartitionSpec as P

ADIABATIC = 4.0 / 3.0
INNER_RADIUS = 1.0
OUTER_RADIUS = 2.0
COURANT = 0.4
GRAVITY_KICK = 0.004
MINIMUM_DENSITY = 0.05
PRESSURE_FLOOR = 0.01
MESH = pl.DeviceIdType.MESH
TILE = 8
PAD = 8
DEPTH = 8
LINE = 2 * DEPTH
TOP = 4


def step_sizes(radial_total, phi_total, theta_total):
    theta_step = math.pi / theta_total
    phi_step = 2.0 * math.pi / phi_total
    polar_width = INNER_RADIUS * math.sin(0.5 * theta_step) * phi_step
    radial_step = min(2.0 * polar_width, (OUTER_RADIUS - INNER_RADIUS) / radial_total)
    timestep = COURANT * min(radial_step, polar_width)
    return (radial_step, theta_step, phi_step, timestep)


def angle_tables(theta_cells, theta_step):
    step = np.float32(theta_step)
    centre = (np.arange(theta_cells, dtype=np.float32) + np.float32(0.5)) * step
    face = np.arange(theta_cells + 1, dtype=np.float32) * step
    sine = np.sin(centre.astype(np.float64))
    cosine = np.cos(centre.astype(np.float64))
    face_sine = np.sin(face.astype(np.float64))
    face_sine[-1] = 0.0
    zero = np.zeros(theta_cells)
    upper = 0.5 * face_sine[1:] / theta_step
    rows = [sine, upper, cosine / sine, 1.0 / sine, zero, zero, zero, zero]
    return np.stack(rows).astype(np.float32)


def half_slope(below, above):
    high, low = jnp.maximum(below, 0.0), jnp.minimum(below, 0.0)
    return 0.5 * jnp.maximum(jnp.minimum(above, high), low)


def thermo(q):
    density = jnp.maximum(q[0], MINIMUM_DENSITY)
    inverse = 1.0 / density
    kinetic = 0.5 * (q[1] * q[1] + q[2] * q[2] + q[3] * q[3]) * inverse
    pressure = jnp.maximum((ADIABATIC - 1.0) * (q[4] - kinetic), PRESSURE_FLOOR * density)
    return density, inverse, pressure


def physical(q, component):
    _, inverse, pressure = thermo(q)
    normal = q[component] * inverse
    squared = ADIABATIC * pressure * inverse
    return normal, pressure, jnp.abs(normal) + squared * lax.rsqrt(squared)


def flux(left, right, component, half_area):
    left_v, left_p, left_a = physical(left, component)
    right_v, right_p, right_a = physical(right, component)
    signal = jnp.maximum(left_a, right_a)
    left_w = half_area * (left_v + signal)
    right_w = half_area * (right_v - signal)
    out = [a * left_w + b * right_w for a, b in zip(left, right)]
    out[component] = out[component] + half_area * (left_p + right_p)
    out[4] = out[4] + half_area * (left_p * left_v + right_p * right_v)
    return out


def each(low, high, step):
    lax.fori_loop(low, high, lambda r, _: (step(r), 0)[1], 0)


def each_pair(low, high, step):
    def both(i):
        step(2 * i)
        step(2 * i + 1)

    each(low // 2, high // 2, both)


def stencils(sizes, extent, slab, table, ends, radial):
    radial_step, theta_step, phi_step, _ = sizes
    variables, rows, cells, lanes = extent
    tiles = cells // TILE
    shape = (TILE, lanes)
    sub = lax.broadcasted_iota(jnp.int32, shape, 0)
    lane_tile = lax.broadcasted_iota(jnp.int32, shape, 1)
    is_last = lane_tile == lanes - 1
    is_top, is_bottom = sub == TILE - 1, sub == 0

    def spread(value):
        return jnp.broadcast_to(value, shape)

    def radius_of(index):
        index = jnp.full(shape, slab * rows + index, jnp.int32).astype(jnp.float32)
        return INNER_RADIUS + (index + 0.5) * radial_step

    def radial_faces(buffer, low, count, tile):
        where = pl.ds(PAD + TILE * tile, TILE)
        lefts = [[] for _ in range(count)]
        rights = [[] for _ in range(count)]
        for k in range(variables):
            q = [buffer[k, low + j, where, :] for j in range(count + 3)]
            step = [q[j + 1] - q[j] for j in range(count + 2)]
            slope = [half_slope(step[j], step[j + 1]) for j in range(count + 1)]
            for i in range(count):
                lefts[i].append(q[i + 1] + slope[i])
                rights[i].append(q[i + 2] - slope[i + 1])
        out = []
        for i in range(count):
            face = radius_of(low + i) - 0.5 * radial_step
            out.append(flux(lefts[i], rights[i], 1, face * face * (0.5 / radial_step)))
        return out

    def radial_store(buffer, low, count):
        for t in range(tiles):
            for i, face in enumerate(radial_faces(buffer, low, count, t)):
                for k in range(variables):
                    radial[k, low + i, pl.ds(TILE * t, TILE), :] = face[k]

    def theta_part(centre):
        left, right = [], []
        for q in centre:
            after = pltpu.roll(q, lanes - 1, 1)
            above = jnp.where(is_last, 0.0, after - q)
            below = pltpu.roll(above, 1, 1)
            slope = half_slope(below, above)
            left.append(q + slope)
            right.append(pltpu.roll(q - slope, lanes - 1, 1))
        upper = flux(left, right, 2, spread(table[1:2, :]))
        return [pltpu.roll(f, 1, 1) - f for f in upper]

    def phi_ends(own, other, pulled):
        def column_at(k, buffer, side, cell):
            return pulled(k, side, cell, buffer is other, buffer[side, k, cell])

        left, right = [], []
        for k in range(variables):
            a, b = (column_at(k, other, 1, cell) for cell in range(2))
            c, d = (column_at(k, own, 0, cell) for cell in range(2))
            left.append(b + half_slope(b - a, c - b))
            right.append(c - half_slope(c - b, d - c))
            a = column_at(k, own, 1, 1)
            b, c = (column_at(k, other, 0, cell) for cell in range(2))
            ends[1, k] = b - half_slope(b - a, c - b)
        for k, f in enumerate(flux(left, right, 3, 0.5 / phi_step)):
            ends[0, k] = f

    def phi_part(buffer, r):
        left, right = [[] for _ in range(tiles)], [[] for _ in range(tiles)]
        for k in range(variables):
            turned = []
            for t in range(tiles):
                start = PAD + TILE * t
                a, b, c = (
                    buffer[k, r + 2, pl.ds(start + offset, TILE), :] for offset in (-1, 0, 1)
                )
                slope = half_slope(b - a, c - b)
                left[t].append(b + slope)
                turned.append(pltpu.roll(b - slope, TILE - 1, 0))
            turned.append(spread(ends[1, k, pl.ds(r, 1), :]))
            for t in range(tiles):
                right[t].append(jnp.where(is_top, turned[t + 1], turned[t]))
        upper = [flux(left[t], right[t], 3, 0.5 / phi_step) for t in range(tiles)]
        out = [[] for _ in range(tiles)]
        for k in range(variables):
            before = spread(ends[0, k, pl.ds(r, 1), :])
            for t in range(tiles):
                turned = pltpu.roll(upper[t][k], 1, 0)
                out[t].append(jnp.where(is_bottom, before, turned) - upper[t][k])
                before = turned
        return out

    def sources(centre, inverse_r):
        density, inverse, pressure = thermo(centre)
        vr, vt, vp = (centre[m] * inverse for m in (1, 2, 3))
        cot = spread(table[2:3, :])
        swirl = density * vp * vp
        return density, [
            (2.0 * pressure + density * vt * vt + swirl) * inverse_r,
            ((pressure + swirl) * cot - density * vr * vt) * inverse_r,
            -density * vp * (vr + vt * cot) * inverse_r,
        ]

    def centre_at(buffer, r, tile):
        return [
            buffer[k, r + 2, pl.ds(PAD + TILE * tile, TILE), :] for k in range(variables)
        ]

    return types.SimpleNamespace(
        spread=spread,
        radius_of=radius_of,
        radial_faces=radial_faces,
        radial_store=radial_store,
        theta_part=theta_part,
        phi_ends=phi_ends,
        phi_part=phi_part,
        sources=sources,
        centre_at=centre_at,
    )


def kernel(
    sizes,
    counts,
    core_ref,
    table_ref,
    input_ref,
    first,
    second,
    pull,
    table,
    mass_ref,
    ends,
    edge_one,
    halo_one,
    edge_two,
    halo_two,
    edge_inside,
    halo_inside,
    edge_end,
    halo_end,
    radial,
    part,
    slab_part,
    got_part,
    got,
    got_above,
    core,
    far,
    told,
    load_sem,
    radial_send,
    radial_recv,
    phi_send,
    phi_recv,
    part_send,
    part_recv,
    slab_send,
    slab_recv,
    above_recv,
):
    radial_step, theta_step, phi_step, timestep = sizes
    slabs, wedges = counts
    variables, rows, cells, lanes = input_ref.shape
    tiles = cells // TILE
    strength = GRAVITY_KICK / timestep
    slab, wedge = lax.axis_index("radial"), lax.axis_index("phi")
    has_up, has_down = slab < slabs - 1, slab > 0
    shape = (TILE, lanes)

    load = pltpu.make_async_copy(
        input_ref, first.at[:, pl.ds(2, rows), pl.ds(PAD, cells), :], load_sem.at[0]
    )
    load.start()
    load_table = pltpu.make_async_copy(table_ref, table, load_sem.at[1])
    load_table.start()
    load_core = pltpu.make_async_copy(core_ref, core, load_sem.at[2])
    load_core.start()

    def radial_peer(jump):
        return (slab + jump, wedge)

    def phi_peer(jump):
        return (slab, lax.rem(wedge + jump, wedges))

    barrier = pltpu.get_barrier_semaphore()
    x, z, c = slab // LINE, (slab // 2) % DEPTH, slab % 2
    level = jnp.where(z < TOP, z, TOP + x)
    rank = jnp.where(z < TOP, 2 * x + c, 2 * (z - TOP) + c)
    span, levels = slabs // DEPTH, DEPTH
    turns = jnp.logical_and(slab % LINE == 0, has_down)
    turned_last = slab % LINE == LINE - 1
    turned_to = jnp.logical_and(turned_last, has_up)

    def signal(semaphore, peer):
        pl.semaphore_signal(semaphore, inc=1, device_id=peer, device_id_type=MESH)

    def each_slab(low, high, step):
        def one_level(at):
            for i in range(span):
                spread_out = LINE * (i // 2) + 2 * at + i % 2
                step(jnp.where(at < TOP, spread_out, LINE * (at - TOP) + LINE // 2 + i))

        each(low, high, one_level)

    def greet(v):
        signal(barrier, (v, wedge))

    def greet_level(v):
        pl.when(jnp.logical_or(v < slab, v == slab + 1))(lambda: greet(v))

    def greet_outer(v):
        known = jnp.logical_or(v % LINE != LINE - 1, v == slab - 1)
        pl.when(known)(lambda: greet(v))

    for j in range(1, wedges):
        signal(barrier, phi_peer(j))
    pl.when(jnp.logical_and(z > 0, jnp.logical_and(z <= TOP, c == 0)))(lambda: greet(slab - 1))
    pl.when(turned_to)(lambda: greet(slab + 1))
    each_slab(level, level + 1, greet_level)
    each_slab(level + 1, levels, greet_outer)
    inside = jnp.where(z < TOP, 2 * c, jnp.where(rank > 0, 1, 0))
    inside = jnp.where(turned_last, jnp.where(has_up, 2, 1), span * level + span - 1 - rank + inside)
    greeted = (wedges - 1) + inside + jnp.where(turns, 1, 0)
    further = slabs // LINE - 1 - x
    heard = (
        jnp.where(z < TOP, (TOP - 1 - z) * 2 * (further + 1), 0),
        jnp.where(z < TOP, (DEPTH - TOP) * 2 * (further + 1), span * further),
    )

    load.wait()
    load_table.wait()
    load_core.wait()

    def remote(src, dst, send, recv, peer):
        return pltpu.make_async_remote_copy(
            src_ref=src, dst_ref=dst, send_sem=send, recv_sem=recv, device_id=peer,
            device_id_type=MESH,
        )

    def radial_copies(buffer, section):
        where, slot = pl.ds(PAD, cells), 2 * section
        up = remote(
            buffer.at[:, pl.ds(rows, 2), where, :], buffer.at[:, pl.ds(0, 2), where, :],
            radial_send.at[0], radial_recv.at[slot], radial_peer(1),
        )
        down = remote(
            buffer.at[:, pl.ds(2, 2), where, :], buffer.at[:, pl.ds(rows + 2, 2), where, :],
            radial_send.at[1], radial_recv.at[slot + 1], radial_peer(-1),
        )
        return up, down

    def radial_start(copies):
        up, down = copies
        pl.when(has_up)(up.start)
        pl.when(has_down)(down.start)

    def radial_sent(copies):
        up, down = copies
        pl.when(has_up)(up.wait_send)
        pl.when(has_down)(down.wait_send)

    def radial_land(copies):
        up, down = copies
        pl.when(has_down)(up.wait_recv)
        pl.when(has_up)(down.wait_recv)

    def bottom_end(buffer):
        for t in range(tiles):
            where = pl.ds(PAD + TILE * t, TILE)
            value = buffer[:, 2, where, :]
            buffer[:, 0, where, :] = value
            buffer[:, 1, where, :] = value

    def top_end(buffer):
        for t in range(tiles):
            where = pl.ds(PAD + TILE * t, TILE)
            value = buffer[:, rows + 1, where, :]
            buffer[:, rows + 2, where, :] = value
            buffer[:, rows + 3, where, :] = value

    sides = ((0, PAD, PAD + cells, wedges - 1), (1, PAD + cells - 2, PAD - 2, 1))

    def phi_copies(source, target, slot):
        return [
            remote(
                source.at[side], target.at[side], phi_send.at[slot], phi_recv.at[slot],
                phi_peer(jump),
            )
            for side, _, _, jump in sides
        ]

    def phi_both(source, target, slot):
        return remote(source, target, phi_send.at[slot], phi_recv.at[slot], phi_peer(1))

    def phi_pack(buffer, full, piece, begin, count):
        for side, start, _, _ in sides:
            for i in range(count):
                value = buffer[:, 2 + begin + i, pl.ds(start, 2), :]
                piece[side, :, :, i, :] = value
                if full is not None:
                    full[side, :, :, begin + i, :] = value

    def phi_unpack(buffer, full, piece, begin, count):
        for side, _, start, _ in sides:
            for i in range(count):
                value = piece[side, :, :, i, :]
                buffer[:, 2 + begin + i, pl.ds(start, 2), :] = value
                if full is not None:
                    full[side, :, :, begin + i, :] = value

    lane = lax.broadcasted_iota(jnp.int32, (rows, lanes), 1)
    line = lax.broadcasted_iota(jnp.int32, (rows, lanes), 0)
    column = jnp.sum(first[0, pl.ds(2, rows), pl.ds(PAD, cells), :], axis=1)
    column = jnp.sum(column * table[0:1, :], axis=1, keepdims=True)
    centres = INNER_RADIUS + (
        (slab * rows + line).astype(jnp.float32) + 0.5
    ) * radial_step
    column = column * centres * centres * (radial_step * theta_step * phi_step)
    part[...] = jnp.sum(jnp.where(lane == line, column, 0.0), axis=0, keepdims=True)
    phi_pack(first, None, edge_one, 0, rows)

    on = stencils(sizes, input_ref.shape, slab, table, ends, radial)

    def early_one(r):
        inverse_r = 1.0 / on.radius_of(r)
        around = inverse_r * on.spread(table[3:4, :]) * timestep
        for t in range(tiles):
            centre = on.centre_at(first, r, t)
            total = [c + d * around for c, d in zip(centre, on.theta_part(centre))]
            _, source = on.sources(centre, inverse_r)
            for m in range(3):
                total[m + 1] = total[m + 1] + timestep * source[m]
            for k in range(variables):
                second[k, r + 2, pl.ds(PAD + TILE * t, TILE), :] = total[k]

    def late_one(r):
        inverse_r = 1.0 / on.radius_of(r)
        around = inverse_r * on.spread(table[3:4, :]) * timestep
        along = inverse_r * inverse_r * timestep
        for t, part_of in enumerate(on.phi_part(first, r)):
            into = pl.ds(TILE * t, TILE)
            where = pl.ds(PAD + TILE * t, TILE)
            for k in range(variables):
                across = radial[k, r, into, :] - radial[k, r + 1, into, :]
                second[k, r + 2, where, :] = (
                    second[k, r + 2, where, :] + part_of[k] * around + across * along
                )

    pl.semaphore_wait(barrier, greeted)

    def reply(v):
        pl.when(v < slab)(lambda: signal(far.at[jnp.where(z < TOP, 0, 1)], (v, wedge)))

    part_copies = [
        remote(part, got_part.at[j], part_send.at[0], part_recv.at[0], phi_peer(j))
        for j in range(1, wedges)
    ]
    others = pl.ds(1, wedges - 1)
    part_all = remote(
        got_part.at[others], got_part.at[others], part_send.at[0], part_recv.at[0], phi_peer(1)
    )
    first_radial, second_radial = radial_copies(first, 0), radial_copies(second, 1)
    first_phi = phi_copies(edge_one, halo_one, 0)
    inside_phi = phi_copies(edge_inside, halo_inside, 1)
    for copy in part_copies:
        copy.start()
    radial_start(first_radial)
    for copy in first_phi:
        copy.start()

    pl.when(slab % LINE == LINE - 2)(lambda: signal(told, (slab + 1, wedge)))

    @pl.when(jnp.logical_not(turned_last))
    def _():
        each_slab(0, level, reply)

    got_part[0] = part[...]
    each_pair(0, rows, early_one)
    each(0, 2, lambda i: on.radial_store(first, 2 + 2 * i, 2))
    on.radial_store(first, 6, 1)

    @pl.when(turned_last)
    def _():
        pl.semaphore_wait(told, 1)
        each_slab(0, level, reply)

    part_all.wait_recv()
    shells = jnp.zeros((1, lanes), jnp.float32)
    for w in range(wedges):
        shells = shells + got_part[lax.rem(wedge + wedges - w, wedges)]
    slab_part[...] = shells

    def slab_copy(source, target):
        return remote(
            slab_part, got.at[source], slab_send.at[0], slab_recv.at[0], (target, wedge),
        )

    def slab_all(count):
        ref = got.at[pl.ds(0, count)]
        return remote(ref, ref, slab_send.at[0], slab_recv.at[0], radial_peer(0))

    def by_slab(low, high, step):
        if high - low == 1:
            step(low)
            return
        middle = (low + high) // 2
        pl.when(slab < middle)(lambda: by_slab(low, middle, step))
        pl.when(slab >= middle)(lambda: by_slab(middle, high, step))

    def slab_start(v):
        pl.when(v > slab)(lambda: slab_copy(slab, v).start())

    above_copy = remote(
        slab_part, got_above, slab_send.at[0], above_recv.at[0], radial_peer(-1)
    )
    each_slab(0, level + 1, slab_start)
    pl.when(has_down)(above_copy.start)

    def send_out():
        for at, low, high in ((0, level + 1, TOP), (1, jnp.maximum(level + 1, TOP), levels)):
            @pl.when(heard[at] > 0)
            def _():
                pl.semaphore_wait(far.at[at], heard[at])
                each_slab(low, high, slab_start)

    def edge_rows(number, high):
        up, down = first_radial
        second_up, second_down = second_radial
        begin = jnp.where(high, rows - 2, 0)
        low = jnp.logical_not(high)
        pl.when(jnp.logical_and(high, has_up))(down.wait_recv)
        pl.when(jnp.logical_and(low, has_down))(up.wait_recv)
        pl.when(jnp.logical_and(high, jnp.logical_not(has_up)))(lambda: top_end(first))
        pl.when(jnp.logical_and(low, jnp.logical_not(has_down)))(lambda: bottom_end(first))
        on.radial_store(first, jnp.where(high, rows - 1, 0), 2)
        each(begin, begin + 2, late_one)

        @pl.when(jnp.logical_and(high, has_up))
        def _():
            up.wait_send()
            second_up.start()

        @pl.when(jnp.logical_and(low, has_down))
        def _():
            down.wait_send()
            second_down.start()

        phi_pack(second, edge_two, edge_end.at[number], begin, 2)
        for copy in phi_copies(edge_end.at[number], halo_end.at[number], 2 + number):
            copy.start()

    phi_both(edge_one, halo_one, 0).wait_recv()
    phi_unpack(first, None, halo_one, 0, rows)
    on.phi_ends(edge_one, halo_one, lambda k, side, cell, other, value: value)
    each(2, rows - 2, late_one)
    phi_pack(second, edge_two, edge_inside, 2, rows - 4)
    for copy in inside_phi:
        copy.start()
    edge_rows(0, c == 0)
    pl.when(turns)(send_out)
    edge_rows(1, c == 1)
    pl.when(jnp.logical_not(turns))(send_out)

    after = jnp.where(lane < line, 1.0, jnp.where(lane == line, 0.5, 0.0))
    within = jnp.sum(after * slab_part[...], axis=1, keepdims=True)
    whole = jnp.sum(jnp.where(line >= 0, slab_part[...], 0.0), axis=1, keepdims=True)

    phi_both(edge_inside, halo_inside, 1).wait_recv()
    phi_unpack(second, halo_two, halo_inside, 2, rows - 4)
    for number in range(2):
        begin = jnp.where(c == number, rows - 2, 0)
        phi_both(edge_end.at[number], halo_end.at[number], 2 + number).wait_recv()
        phi_unpack(second, halo_two, halo_end.at[number], begin, 2)
    radial_land(second_radial)

    part_all.wait_send()
    phi_both(edge_one, halo_one, 0).wait_send()
    phi_both(edge_inside, halo_inside, 1).wait_send()
    for number in range(2):
        phi_both(edge_end.at[number], halo_end.at[number], 2 + number).wait_send()
    radial_sent(second_radial)
    by_slab(0, slabs, lambda s: slab_all(slabs - max(s, 1)).wait_send())
    pl.when(has_up)(above_copy.wait_recv)
    by_slab(0, slabs, lambda s: slab_all(s).wait_recv() if s else None)
    sums = [jnp.zeros((1, lanes), jnp.float32) for _ in range(4)]
    for v in range(slabs - 1):
        sums[v % 4] = sums[v % 4] + jnp.where(slab > v, got[v], 0.0)
    before = jnp.broadcast_to((sums[0] + sums[1]) + (sums[2] + sums[3]), (rows, lanes))
    before = core[0] + jnp.sum(before, axis=1, keepdims=True)
    inner = jnp.where(lane > line, 1.0, jnp.where(lane == line, 0.5, 0.0))
    inner = jnp.sum(inner * got[jnp.maximum(slab - 1, 0)], axis=1, keepdims=True)
    outer = jnp.sum(after * got_above[...], axis=1, keepdims=True)
    wide = jnp.zeros((rows, lanes), jnp.float32)
    enclosed = before + within + wide
    mass_ref[...] = jnp.sum(jnp.where(lane == line, enclosed, 0.0), axis=0, keepdims=True)[:, :rows]
    for i, inside in ((0, before - inner), (1, before + within), (2, before + whole + outer)):
        at = centres + (i - 1) * rows * radial_step
        pull[pl.ds(8 * i, 8), :] = strength * (inside + wide) / (at * at)

    def pulled(row, start):
        where = pl.ds(start, TILE)
        gravity = timestep * on.spread(pull[pl.ds(row + 6, 1), :])
        density = jnp.maximum(first[0, row, where, :], MINIMUM_DENSITY)
        second[1, row, where, :] = second[1, row, where, :] - density * gravity
        second[4, row, where, :] = second[4, row, where, :] - first[1, row, where, :] * gravity

    def pulled_row(row):
        for t in range(-1, tiles + 1):
            pulled(row, PAD + TILE * t)

    each_pair(0, rows + 4, pulled_row)
    pl.when(jnp.logical_not(has_down))(lambda: bottom_end(second))
    pl.when(jnp.logical_not(has_up))(lambda: top_end(second))

    tug = timestep * pull[pl.ds(TILE, rows), :]

    def pulled_end(k, side, cell, other, value):
        begin = halo_one if other else edge_one
        if k == 1:
            value = value - jnp.maximum(begin[side, 0, cell], MINIMUM_DENSITY) * tug
        if k == 4:
            value = value - begin[side, 1, cell] * tug
        return value

    on.phi_ends(edge_two, halo_two, pulled_end)


def finish(
    sizes,
    first,
    second,
    pull,
    table,
    mass,
    ends,
    out_ref,
    mass_ref,
    out,
    radial,
    sem,
):
    timestep = sizes[3]
    variables, rows, cells, lanes = out.shape
    tiles = cells // TILE
    slab = lax.axis_index("radial")
    on = stencils(sizes, out.shape, slab, table, ends, radial)
    save_mass = pltpu.make_async_copy(mass, mass_ref, sem.at[1])
    save_mass.start()

    def section_two(r):
        inverse_r = 1.0 / on.radius_of(r)
        scale = 0.5 * timestep
        around = inverse_r * on.spread(table[3:4, :]) * scale
        along = inverse_r * inverse_r * scale
        gravity = on.spread(pull[pl.ds(r + 8, 1), :])
        phi = on.phi_part(second, r)
        for t in range(tiles):
            into = pl.ds(TILE * t, TILE)
            where = pl.ds(PAD + TILE * t, TILE)
            centre = on.centre_at(second, r, t)
            theta = on.theta_part(centre)
            density, source = on.sources(centre, inverse_r)
            source[0] = source[0] - density * gravity
            source.append(-centre[1] * gravity)
            total = [
                0.5 * (first[k, r + 2, where, :] + centre[k])
                + (theta[k] + phi[t][k]) * around
                + (radial[k, r, into, :] - radial[k, r + 1, into, :]) * along
                for k in range(variables)
            ]
            for m in range(4):
                total[m + 1] = total[m + 1] + scale * source[m]
            for k in range(variables):
                out[k, r, into, :] = total[k]

    def save(i):
        where = (slice(None), pl.ds(2 * i, 2))
        return pltpu.make_async_copy(out.at[where], out_ref.at[where], sem.at[0])

    def two(i):
        section_two(2 * i)
        section_two(2 * i + 1)
        save(i).start()

    each(0, (rows + 1) // 3, lambda i: on.radial_store(second, 3 * i, 3))
    each(0, rows // 2, two)
    pltpu.make_async_copy(out, out_ref, sem.at[0]).wait()
    save_mass.wait()


def body(conserved, core_mass):
    variables, rows, cells, lanes = conserved.shape
    slabs, wedges = lax.axis_size("radial"), lax.axis_size("phi")
    sizes = step_sizes(rows * slabs, cells * wedges, lanes)
    table = jnp.asarray(angle_tables(lanes, sizes[1]))
    padded = (variables, rows + 4, cells + 2 * PAD, lanes)
    vmem = pl.BlockSpec(memory_space=pltpu.VMEM)
    dma = pltpu.SemaphoreType.DMA
    first, second, pull, table, mass, ends = pl.pallas_call(
        functools.partial(kernel, sizes, (slabs, wedges)),
        out_shape=(
            pltpu.VMEM(padded, jnp.float32),
            pltpu.VMEM(padded, jnp.float32),
            pltpu.VMEM((3 * TILE, lanes), jnp.float32),
            pltpu.VMEM((TILE, lanes), jnp.float32),
            pltpu.VMEM((1, rows), jnp.float32),
            pltpu.VMEM((2, variables, rows, lanes), jnp.float32),
        ),
        in_specs=[pl.BlockSpec(memory_space=pl.ANY)] * 3,
        out_specs=(vmem,) * 6,
        scratch_shapes=[
            *[pltpu.VMEM((2, variables, 2, rows, lanes), jnp.float32)] * 4,
            *[pltpu.VMEM((2, variables, 2, rows - 4, lanes), jnp.float32)] * 2,
            *[pltpu.VMEM((2, 2, variables, 2, 2, lanes), jnp.float32)] * 2,
            pltpu.VMEM((variables, rows + 1, cells, lanes), jnp.float32),
            pltpu.VMEM((1, lanes), jnp.float32),
            pltpu.VMEM((1, lanes), jnp.float32),
            pltpu.VMEM((wedges, 1, lanes), jnp.float32),
            pltpu.VMEM((slabs, 1, lanes), jnp.float32),
            pltpu.VMEM((1, lanes), jnp.float32),
            pltpu.SMEM((1,), jnp.float32),
            pltpu.SemaphoreType.REGULAR((2,)),
            pltpu.SemaphoreType.REGULAR,
            dma((3,)),
            dma((2,)),
            dma((4,)),
            dma((4,)),
            dma((4,)),
            dma((1,)),
            dma((1,)),
            dma((1,)),
            dma((1,)),
            dma((1,)),
        ],
        compiler_params=pltpu.CompilerParams(collective_id=0, has_side_effects=True),
    )(core_mass, table, conserved)
    advanced, mass = pl.pallas_call(
        functools.partial(finish, sizes),
        out_shape=(
            jax.ShapeDtypeStruct(conserved.shape, jnp.float32),
            jax.ShapeDtypeStruct((1, rows), jnp.float32),
        ),
        in_specs=[vmem] * 6,
        out_specs=(pl.BlockSpec(memory_space=pltpu.HBM),) * 2,
        scratch_shapes=[
            pltpu.VMEM(conserved.shape, jnp.float32),
            pltpu.VMEM((variables, rows + 1, cells, lanes), jnp.float32),
            dma((2,)),
        ],
        compiler_params=pltpu.CompilerParams(vmem_limit_bytes=16 * 1024 * 1024),
    )(first, second, pull, table, mass, ends)
    return advanced, mass.reshape(rows)


def solution(mesh):
    in_specs = (P(None, "radial", "phi", None), P())
    out_specs = (P(None, "radial", "phi", None), P("radial"))
    return jax.shard_map(body, mesh=mesh, in_specs=in_specs, out_specs=out_specs, check_vma=False)
```

```python
import functools
import math
import types

import jax
import jax.numpy as jnp
import numpy as np
from jax import lax
from jax.experimental import pallas as pl
from jax.experimental.pallas import tpu as pltpu
from jax.sharding import PartitionSpec as P

ADIABATIC = 4.0 / 3.0
INNER_RADIUS = 1.0
OUTER_RADIUS = 2.0
COURANT = 0.4
GRAVITY_KICK = 0.004
MINIMUM_DENSITY = 0.05
PRESSURE_FLOOR = 0.01
MESH = pl.DeviceIdType.MESH
TILE = 8
PAD = 8
DEPTH = 8
LINE = 2 * DEPTH
STEP = 4
TOP = 4


def step_sizes(radial_total, phi_total, theta_total):
    theta_step = math.pi / theta_total
    phi_step = 2.0 * math.pi / phi_total
    polar_width = INNER_RADIUS * math.sin(0.5 * theta_step) * phi_step
    radial_step = min(2.0 * polar_width, (OUTER_RADIUS - INNER_RADIUS) / radial_total)
    timestep = COURANT * min(radial_step, polar_width)
    return (radial_step, theta_step, phi_step, timestep)


def angle_tables(theta_cells, theta_step):
    step = np.float32(theta_step)
    centre = (np.arange(theta_cells, dtype=np.float32) + np.float32(0.5)) * step
    face = np.arange(theta_cells + 1, dtype=np.float32) * step
    sine = np.sin(centre.astype(np.float64))
    cosine = np.cos(centre.astype(np.float64))
    face_sine = np.sin(face.astype(np.float64))
    face_sine[-1] = 0.0
    zero = np.zeros(theta_cells)
    upper = 0.5 * face_sine[1:] / theta_step
    rows = [sine, upper, cosine / sine, 1.0 / sine, zero, zero, zero, zero]
    return np.stack(rows).astype(np.float32)


def half_slope(below, above):
    high, low = jnp.maximum(below, 0.0), jnp.minimum(below, 0.0)
    return 0.5 * jnp.maximum(jnp.minimum(above, high), low)


def thermo(q):
    density = jnp.maximum(q[0], MINIMUM_DENSITY)
    inverse = 1.0 / density
    kinetic = 0.5 * (q[1] * q[1] + q[2] * q[2] + q[3] * q[3]) * inverse
    pressure = jnp.maximum((ADIABATIC - 1.0) * (q[4] - kinetic), PRESSURE_FLOOR * density)
    return density, inverse, pressure


def physical(q, component):
    _, inverse, pressure = thermo(q)
    normal = q[component] * inverse
    squared = ADIABATIC * pressure * inverse
    return normal, pressure, jnp.abs(normal) + squared * lax.rsqrt(squared)


def flux(left, right, component, half_area):
    left_v, left_p, left_a = physical(left, component)
    right_v, right_p, right_a = physical(right, component)
    signal = jnp.maximum(left_a, right_a)
    left_w = half_area * (left_v + signal)
    right_w = half_area * (right_v - signal)
    out = [a * left_w + b * right_w for a, b in zip(left, right)]
    out[component] = out[component] + half_area * (left_p + right_p)
    out[4] = out[4] + half_area * (left_p * left_v + right_p * right_v)
    return out


def each(low, high, step):
    lax.fori_loop(low, high, lambda r, _: (step(r), 0)[1], 0)


def each_pair(low, high, step):
    def both(i):
        step(2 * i)
        step(2 * i + 1)

    each(low // 2, high // 2, both)


def stencils(sizes, extent, slab, table, ends, radial):
    radial_step, theta_step, phi_step, _ = sizes
    variables, rows, cells, lanes = extent
    tiles = cells // TILE
    shape = (TILE, lanes)
    sub = lax.broadcasted_iota(jnp.int32, shape, 0)
    lane_tile = lax.broadcasted_iota(jnp.int32, shape, 1)
    is_last = lane_tile == lanes - 1
    is_top, is_bottom = sub == TILE - 1, sub == 0

    def spread(value):
        return jnp.broadcast_to(value, shape)

    def radius_of(index):
        index = jnp.full(shape, slab * rows + index, jnp.int32).astype(jnp.float32)
        return INNER_RADIUS + (index + 0.5) * radial_step

    def radial_faces(buffer, low, count, tile):
        where = pl.ds(PAD + TILE * tile, TILE)
        lefts = [[] for _ in range(count)]
        rights = [[] for _ in range(count)]
        for k in range(variables):
            q = [buffer[k, low + j, where, :] for j in range(count + 3)]
            step = [q[j + 1] - q[j] for j in range(count + 2)]
            slope = [half_slope(step[j], step[j + 1]) for j in range(count + 1)]
            for i in range(count):
                lefts[i].append(q[i + 1] + slope[i])
                rights[i].append(q[i + 2] - slope[i + 1])
        out = []
        for i in range(count):
            face = radius_of(low + i) - 0.5 * radial_step
            out.append(flux(lefts[i], rights[i], 1, face * face * (0.5 / radial_step)))
        return out

    def radial_store(buffer, low, count):
        for t in range(tiles):
            for i, face in enumerate(radial_faces(buffer, low, count, t)):
                for k in range(variables):
                    radial[k, low + i, pl.ds(TILE * t, TILE), :] = face[k]

    def theta_part(centre):
        left, right = [], []
        for q in centre:
            after = pltpu.roll(q, lanes - 1, 1)
            above = jnp.where(is_last, 0.0, after - q)
            below = pltpu.roll(above, 1, 1)
            slope = half_slope(below, above)
            left.append(q + slope)
            right.append(pltpu.roll(q - slope, lanes - 1, 1))
        upper = flux(left, right, 2, spread(table[1:2, :]))
        return [pltpu.roll(f, 1, 1) - f for f in upper]

    def phi_ends(own, other, pulled):
        def column_at(k, buffer, side, cell):
            return pulled(k, side, cell, buffer is other, buffer[side, k, cell])

        left, right = [], []
        for k in range(variables):
            a, b = (column_at(k, other, 1, cell) for cell in range(2))
            c, d = (column_at(k, own, 0, cell) for cell in range(2))
            left.append(b + half_slope(b - a, c - b))
            right.append(c - half_slope(c - b, d - c))
            a = column_at(k, own, 1, 1)
            b, c = (column_at(k, other, 0, cell) for cell in range(2))
            ends[1, k] = b - half_slope(b - a, c - b)
        for k, f in enumerate(flux(left, right, 3, 0.5 / phi_step)):
            ends[0, k] = f

    def phi_part(buffer, r):
        left, right = [[] for _ in range(tiles)], [[] for _ in range(tiles)]
        for k in range(variables):
            turned = []
            for t in range(tiles):
                start = PAD + TILE * t
                a, b, c = (
                    buffer[k, r + 2, pl.ds(start + offset, TILE), :] for offset in (-1, 0, 1)
                )
                slope = half_slope(b - a, c - b)
                left[t].append(b + slope)
                turned.append(pltpu.roll(b - slope, TILE - 1, 0))
            turned.append(spread(ends[1, k, pl.ds(r, 1), :]))
            for t in range(tiles):
                right[t].append(jnp.where(is_top, turned[t + 1], turned[t]))
        upper = [flux(left[t], right[t], 3, 0.5 / phi_step) for t in range(tiles)]
        out = [[] for _ in range(tiles)]
        for k in range(variables):
            before = spread(ends[0, k, pl.ds(r, 1), :])
            for t in range(tiles):
                turned = pltpu.roll(upper[t][k], 1, 0)
                out[t].append(jnp.where(is_bottom, before, turned) - upper[t][k])
                before = turned
        return out

    def sources(centre, inverse_r):
        density, inverse, pressure = thermo(centre)
        vr, vt, vp = (centre[m] * inverse for m in (1, 2, 3))
        cot = spread(table[2:3, :])
        swirl = density * vp * vp
        return density, [
            (2.0 * pressure + density * vt * vt + swirl) * inverse_r,
            ((pressure + swirl) * cot - density * vr * vt) * inverse_r,
            -density * vp * (vr + vt * cot) * inverse_r,
        ]

    def centre_at(buffer, r, tile):
        return [
            buffer[k, r + 2, pl.ds(PAD + TILE * tile, TILE), :] for k in range(variables)
        ]

    return types.SimpleNamespace(
        spread=spread,
        radius_of=radius_of,
        radial_faces=radial_faces,
        radial_store=radial_store,
        theta_part=theta_part,
        phi_ends=phi_ends,
        phi_part=phi_part,
        sources=sources,
        centre_at=centre_at,
    )


def kernel(
    sizes,
    counts,
    core_ref,
    table_ref,
    input_ref,
    first,
    second,
    pull,
    table,
    mass_ref,
    ends,
    edge_one,
    halo_one,
    edge_two,
    halo_two,
    edge_inside,
    halo_inside,
    edge_end,
    halo_end,
    radial,
    part,
    slab_part,
    got_part,
    got,
    got_above,
    core,
    far,
    told,
    load_sem,
    radial_send,
    radial_recv,
    phi_send,
    phi_recv,
    part_send,
    part_recv,
    slab_send,
    slab_recv,
    above_recv,
):
    radial_step, theta_step, phi_step, timestep = sizes
    slabs, wedges = counts
    variables, rows, cells, lanes = input_ref.shape
    tiles = cells // TILE
    strength = GRAVITY_KICK / timestep
    slab, wedge = lax.axis_index("radial"), lax.axis_index("phi")
    has_up, has_down = slab < slabs - 1, slab > 0
    shape = (TILE, lanes)

    load = pltpu.make_async_copy(
        input_ref, first.at[:, pl.ds(2, rows), pl.ds(PAD, cells), :], load_sem.at[0]
    )
    load.start()
    load_table = pltpu.make_async_copy(table_ref, table, load_sem.at[1])
    load_table.start()
    load_core = pltpu.make_async_copy(core_ref, core, load_sem.at[2])
    load_core.start()

    def radial_peer(jump):
        return (slab + jump, wedge)

    def phi_peer(jump):
        return (slab, lax.rem(wedge + jump, wedges))

    barrier = pltpu.get_barrier_semaphore()
    x, z, c = slab // LINE, (slab // 2) % DEPTH, slab % 2
    level = jnp.where(z < TOP, z, TOP + x)
    rank = jnp.where(z < TOP, 2 * x + c, 2 * (z - TOP) + c)
    span, levels = slabs // DEPTH, DEPTH
    turns = jnp.logical_and(slab % LINE == 0, has_down)
    turned_last = slab % LINE == LINE - 1
    turned_to = jnp.logical_and(turned_last, has_up)

    def signal(semaphore, peer):
        pl.semaphore_signal(semaphore, inc=1, device_id=peer, device_id_type=MESH)

    def each_slab(low, high, step):
        def spread_out(at):
            for i in range(span):
                step(2 * at + LINE * (i // 2) + i % 2, False)

        def block(at):
            for i in range(span):
                last = i // 2 == DEPTH - TOP - 1
                step(LINE * at + (LINE // 2 - LINE * TOP + i), i % 2 == (1 if last else 0))

        each(low, jnp.minimum(high, TOP), spread_out)
        each(jnp.maximum(low, TOP), high, block)

    def greet(v):
        signal(barrier, (v, wedge))

    def near(v):
        return jnp.logical_or(v == slab + 1, v == slab - 1)

    def greet_level(v, later):
        known = jnp.logical_or(v < slab, v == slab + 1)
        known = jnp.logical_and(known, near(v)) if later else known
        pl.when(known)(lambda: greet(v))

    def greet_outer(v, later):
        if later:
            pl.when(near(v))(lambda: greet(v))
        else:
            greet(v)

    for j in range(1, wedges):
        signal(barrier, phi_peer(j))
    pl.when(jnp.logical_and(z > 0, jnp.logical_and(z <= TOP, c == 0)))(lambda: greet(slab - 1))
    pl.when(turned_to)(lambda: greet(slab + 1))
    each_slab(level, level + 1, greet_level)
    each_slab(level + 1, levels, greet_outer)
    inside = jnp.where(z < TOP, 2 * c, jnp.where(rank > 0, 1, 0))
    late = jnp.logical_and(z >= TOP, c == jnp.where(z == DEPTH - 1, 1, 0))
    inside = jnp.where(late, jnp.where(has_up, 2, 1), span * level + span - 1 - rank + inside)
    greeted = (wedges - 1) + inside + jnp.where(turns, 1, 0)
    further = slabs // LINE - 1 - x
    heard = (
        jnp.where(z < TOP, (TOP - 1 - z) * 2 * (further + 1), 0),
        jnp.where(z < TOP, (DEPTH - TOP) * 2 * (further + 1), span * further),
    )


    def remote(src, dst, send, recv, peer):
        return pltpu.make_async_remote_copy(
            src_ref=src, dst_ref=dst, send_sem=send, recv_sem=recv, device_id=peer,
            device_id_type=MESH,
        )

    def radial_copies(buffer, section):
        where, slot = pl.ds(PAD, cells), 2 * section
        up = remote(
            buffer.at[:, pl.ds(rows, 2), where, :], buffer.at[:, pl.ds(0, 2), where, :],
            radial_send.at[0], radial_recv.at[slot], radial_peer(1),
        )
        down = remote(
            buffer.at[:, pl.ds(2, 2), where, :], buffer.at[:, pl.ds(rows + 2, 2), where, :],
            radial_send.at[1], radial_recv.at[slot + 1], radial_peer(-1),
        )
        return up, down

    def radial_sent(copies):
        up, down = copies
        pl.when(has_up)(up.wait_send)
        pl.when(has_down)(down.wait_send)

    def radial_land(copies):
        up, down = copies
        pl.when(has_down)(up.wait_recv)
        pl.when(has_up)(down.wait_recv)

    def bottom_end(buffer):
        for t in range(tiles):
            where = pl.ds(PAD + TILE * t, TILE)
            value = buffer[:, 2, where, :]
            buffer[:, 0, where, :] = value
            buffer[:, 1, where, :] = value

    def top_end(buffer):
        for t in range(tiles):
            where = pl.ds(PAD + TILE * t, TILE)
            value = buffer[:, rows + 1, where, :]
            buffer[:, rows + 2, where, :] = value
            buffer[:, rows + 3, where, :] = value

    sides = ((0, PAD, PAD + cells, wedges - 1), (1, PAD + cells - 2, PAD - 2, 1))

    def phi_copies(source, target, slot):
        return [
            remote(
                source.at[side], target.at[side], phi_send.at[slot], phi_recv.at[slot],
                phi_peer(jump),
            )
            for side, _, _, jump in sides
        ]

    def phi_both(source, target, slot):
        return remote(source, target, phi_send.at[slot], phi_recv.at[slot], phi_peer(1))

    def phi_pack(buffer, full, piece, begin, count):
        for side, start, _, _ in sides:
            for i in range(count):
                value = buffer[:, 2 + begin + i, pl.ds(start, 2), :]
                piece[side, :, :, i, :] = value
                if full is not None:
                    full[side, :, :, begin + i, :] = value

    def phi_unpack(buffer, full, piece, begin, count):
        for side, _, start, _ in sides:
            for i in range(count):
                value = piece[side, :, :, i, :]
                buffer[:, 2 + begin + i, pl.ds(start, 2), :] = value
                if full is not None:
                    full[side, :, :, begin + i, :] = value

    first_radial, second_radial = radial_copies(first, 0), radial_copies(second, 1)
    load.wait()

    @pl.when(turned_last)
    def _():
        pl.semaphore_wait(barrier, greeted)
        pl.when(has_up)(first_radial[0].start)

    load_table.wait()
    load_core.wait()
    lane = lax.broadcasted_iota(jnp.int32, (rows, lanes), 1)
    line = lax.broadcasted_iota(jnp.int32, (rows, lanes), 0)
    column = jnp.sum(first[0, pl.ds(2, rows), pl.ds(PAD, cells), :], axis=1)
    column = jnp.sum(column * table[0:1, :], axis=1, keepdims=True)
    centres = INNER_RADIUS + (
        (slab * rows + line).astype(jnp.float32) + 0.5
    ) * radial_step
    column = column * centres * centres * (radial_step * theta_step * phi_step)
    part[...] = jnp.sum(jnp.where(lane == line, column, 0.0), axis=0, keepdims=True)
    phi_pack(first, None, edge_one, 0, rows)

    on = stencils(sizes, input_ref.shape, slab, table, ends, radial)

    def early_one(r):
        inverse_r = 1.0 / on.radius_of(r)
        around = inverse_r * on.spread(table[3:4, :]) * timestep
        for t in range(tiles):
            centre = on.centre_at(first, r, t)
            total = [c + d * around for c, d in zip(centre, on.theta_part(centre))]
            _, source = on.sources(centre, inverse_r)
            for m in range(3):
                total[m + 1] = total[m + 1] + timestep * source[m]
            for k in range(variables):
                second[k, r + 2, pl.ds(PAD + TILE * t, TILE), :] = total[k]

    def late_one(r):
        inverse_r = 1.0 / on.radius_of(r)
        around = inverse_r * on.spread(table[3:4, :]) * timestep
        along = inverse_r * inverse_r * timestep
        for t, part_of in enumerate(on.phi_part(first, r)):
            into = pl.ds(TILE * t, TILE)
            where = pl.ds(PAD + TILE * t, TILE)
            for k in range(variables):
                across = radial[k, r, into, :] - radial[k, r + 1, into, :]
                second[k, r + 2, where, :] = (
                    second[k, r + 2, where, :] + part_of[k] * around + across * along
                )

    pl.when(jnp.logical_not(turned_last))(lambda: pl.semaphore_wait(barrier, greeted))

    def reply(v, _):
        pl.when(v < slab)(lambda: signal(far.at[jnp.where(z < TOP, 0, 1)], (v, wedge)))

    part_copies = [
        remote(part, got_part.at[j], part_send.at[0], part_recv.at[0], phi_peer(j))
        for j in range(1, wedges)
    ]
    others = pl.ds(1, wedges - 1)
    part_all = remote(
        got_part.at[others], got_part.at[others], part_send.at[0], part_recv.at[0], phi_peer(1)
    )
    first_phi = phi_copies(edge_one, halo_one, 0)
    inside_phi = phi_copies(edge_inside, halo_inside, 1)
    for copy in part_copies:
        copy.start()
    pl.when(jnp.logical_and(has_up, jnp.logical_not(turned_last)))(first_radial[0].start)
    pl.when(has_down)(first_radial[1].start)
    for copy in first_phi:
        copy.start()

    teller = jnp.logical_and(z >= TOP, jnp.logical_not(late))
    pl.when(teller)(lambda: signal(told, (slab + 1 - 2 * c, wedge)))

    @pl.when(jnp.logical_not(late))
    def _():
        each_slab(0, level, reply)

    got_part[0] = part[...]
    each_pair(0, rows, early_one)

    @pl.when(late)
    def _():
        pl.semaphore_wait(told, 1)
        each_slab(0, level, reply)

    each(0, 2, lambda i: on.radial_store(first, 2 + 2 * i, 2))
    on.radial_store(first, 6, 1)
    part_all.wait_recv()
    shells = jnp.zeros((1, lanes), jnp.float32)
    for w in range(wedges):
        shells = shells + got_part[lax.rem(wedge + wedges - w, wedges)]
    slab_part[...] = shells

    def slab_copy(source, target):
        return remote(
            slab_part, got.at[source], slab_send.at[0], slab_recv.at[0], (target, wedge),
        )

    def slab_all(count):
        ref = got.at[pl.ds(0, count)]
        return remote(ref, ref, slab_send.at[0], slab_recv.at[0], radial_peer(0))

    def by_slab(low, high, step):
        if high - low == 1:
            step(low)
            return
        middle = (low + high) // 2
        pl.when(slab < middle)(lambda: by_slab(low, middle, step))
        pl.when(slab >= middle)(lambda: by_slab(middle, high, step))

    def slab_start(v, _):
        pl.when(v > slab)(lambda: slab_copy(slab, v).start())

    above_copy = remote(
        slab_part, got_above, slab_send.at[0], above_recv.at[0], radial_peer(-1)
    )
    each_slab(0, level + 1, slab_start)
    pl.when(has_down)(above_copy.start)

    def send_out():
        for at, low, high in ((0, level + 1, TOP), (1, jnp.maximum(level + 1, TOP), levels)):
            @pl.when(heard[at] > 0)
            def _():
                pl.semaphore_wait(far.at[at], heard[at])
                each_slab(low, high, slab_start)

    def edge_rows(number, high):
        up, down = first_radial
        second_up, second_down = second_radial
        begin = jnp.where(high, rows - 2, 0)
        low = jnp.logical_not(high)
        pl.when(jnp.logical_and(high, has_up))(down.wait_recv)
        pl.when(jnp.logical_and(low, has_down))(up.wait_recv)
        pl.when(jnp.logical_and(high, jnp.logical_not(has_up)))(lambda: top_end(first))
        pl.when(jnp.logical_and(low, jnp.logical_not(has_down)))(lambda: bottom_end(first))
        on.radial_store(first, jnp.where(high, rows - 1, 0), 2)
        each(begin, begin + 2, late_one)

        @pl.when(jnp.logical_and(high, has_up))
        def _():
            up.wait_send()
            second_up.start()

        @pl.when(jnp.logical_and(low, has_down))
        def _():
            down.wait_send()
            second_down.start()

        phi_pack(second, edge_two, edge_end.at[number], begin, 2)
        for copy in phi_copies(edge_end.at[number], halo_end.at[number], 2 + number):
            copy.start()

    phi_both(edge_one, halo_one, 0).wait_recv()
    phi_unpack(first, None, halo_one, 0, rows)
    on.phi_ends(edge_one, halo_one, lambda k, side, cell, other, value: value)
    each(2, rows - 2, late_one)
    phi_pack(second, edge_two, edge_inside, 2, rows - 4)
    for copy in inside_phi:
        copy.start()
    edge_rows(0, c == 0)
    edge_rows(1, c == 1)
    send_out()

    after = jnp.where(lane < line, 1.0, jnp.where(lane == line, 0.5, 0.0))
    within = jnp.sum(after * slab_part[...], axis=1, keepdims=True)
    whole = jnp.sum(jnp.where(line >= 0, slab_part[...], 0.0), axis=1, keepdims=True)

    phi_both(edge_inside, halo_inside, 1).wait_recv()
    phi_unpack(second, halo_two, halo_inside, 2, rows - 4)
    for number in range(2):
        begin = jnp.where(c == number, rows - 2, 0)
        phi_both(edge_end.at[number], halo_end.at[number], 2 + number).wait_recv()
        phi_unpack(second, halo_two, halo_end.at[number], begin, 2)
    radial_land(second_radial)

    part_all.wait_send()
    phi_both(edge_one, halo_one, 0).wait_send()
    phi_both(edge_inside, halo_inside, 1).wait_send()
    for number in range(2):
        phi_both(edge_end.at[number], halo_end.at[number], 2 + number).wait_send()
    radial_sent(second_radial)
    by_slab(0, slabs, lambda s: slab_all(slabs - max(s, 1)).wait_send())
    pl.when(has_up)(above_copy.wait_recv)
    by_slab(0, slabs, lambda s: slab_all(s).wait_recv() if s else None)
    sums = [jnp.zeros((1, lanes), jnp.float32) for _ in range(4)]
    for v in range(slabs - 1):
        sums[v % 4] = sums[v % 4] + jnp.where(slab > v, got[v], 0.0)
    before = jnp.broadcast_to((sums[0] + sums[1]) + (sums[2] + sums[3]), (rows, lanes))
    before = core[0] + jnp.sum(before, axis=1, keepdims=True)
    inner = jnp.where(lane > line, 1.0, jnp.where(lane == line, 0.5, 0.0))
    inner = jnp.sum(inner * got[jnp.maximum(slab - 1, 0)], axis=1, keepdims=True)
    outer = jnp.sum(after * got_above[...], axis=1, keepdims=True)
    wide = jnp.zeros((rows, lanes), jnp.float32)
    enclosed = before + within + wide
    mass_ref[...] = jnp.sum(jnp.where(lane == line, enclosed, 0.0), axis=0, keepdims=True)[:, :rows]
    for i, inside in ((0, before - inner), (1, before + within), (2, before + whole + outer)):
        at = centres + (i - 1) * rows * radial_step
        pull[pl.ds(8 * i, 8), :] = strength * (inside + wide) / (at * at)

    def pulled(row, start):
        where = pl.ds(start, TILE)
        gravity = timestep * on.spread(pull[pl.ds(row + 6, 1), :])
        density = jnp.maximum(first[0, row, where, :], MINIMUM_DENSITY)
        second[1, row, where, :] = second[1, row, where, :] - density * gravity
        second[4, row, where, :] = second[4, row, where, :] - first[1, row, where, :] * gravity

    def pulled_row(row):
        for t in range(-1, tiles + 1):
            pulled(row, PAD + TILE * t)

    each_pair(0, rows + 4, pulled_row)
    pl.when(jnp.logical_not(has_down))(lambda: bottom_end(second))
    pl.when(jnp.logical_not(has_up))(lambda: top_end(second))

    tug = timestep * pull[pl.ds(TILE, rows), :]

    def pulled_end(k, side, cell, other, value):
        begin = halo_one if other else edge_one
        if k == 1:
            value = value - jnp.maximum(begin[side, 0, cell], MINIMUM_DENSITY) * tug
        if k == 4:
            value = value - begin[side, 1, cell] * tug
        return value

    on.phi_ends(edge_two, halo_two, pulled_end)


def finish(
    sizes,
    first,
    second,
    pull,
    table,
    mass,
    ends,
    out_ref,
    mass_ref,
    out,
    radial,
    sem,
):
    timestep = sizes[3]
    variables, rows, cells, lanes = out.shape
    tiles = cells // TILE
    slab = lax.axis_index("radial")
    on = stencils(sizes, out.shape, slab, table, ends, radial)
    save_mass = pltpu.make_async_copy(mass, mass_ref, sem.at[1])
    save_mass.start()

    def section_two(r):
        inverse_r = 1.0 / on.radius_of(r)
        scale = 0.5 * timestep
        around = inverse_r * on.spread(table[3:4, :]) * scale
        along = inverse_r * inverse_r * scale
        gravity = on.spread(pull[pl.ds(r + 8, 1), :])
        phi = on.phi_part(second, r)
        for t in range(tiles):
            into = pl.ds(TILE * t, TILE)
            where = pl.ds(PAD + TILE * t, TILE)
            centre = on.centre_at(second, r, t)
            theta = on.theta_part(centre)
            density, source = on.sources(centre, inverse_r)
            source[0] = source[0] - density * gravity
            source.append(-centre[1] * gravity)
            total = [
                0.5 * (first[k, r + 2, where, :] + centre[k])
                + (theta[k] + phi[t][k]) * around
                + (radial[k, r, into, :] - radial[k, r + 1, into, :]) * along
                for k in range(variables)
            ]
            for m in range(4):
                total[m + 1] = total[m + 1] + scale * source[m]
            for k in range(variables):
                out[k, r, into, :] = total[k]

    def save(i):
        where = (slice(None), pl.ds(STEP * i, STEP))
        return pltpu.make_async_copy(out.at[where], out_ref.at[where], sem.at[0])

    def several(i):
        for j in range(STEP):
            section_two(STEP * i + j)
        save(i).start()

    each(0, (rows + 1) // 3, lambda i: on.radial_store(second, 3 * i, 3))
    each(0, rows // STEP, several)
    pltpu.make_async_copy(out, out_ref, sem.at[0]).wait()
    save_mass.wait()


def body(conserved, core_mass):
    variables, rows, cells, lanes = conserved.shape
    slabs, wedges = lax.axis_size("radial"), lax.axis_size("phi")
    sizes = step_sizes(rows * slabs, cells * wedges, lanes)
    table = jnp.asarray(angle_tables(lanes, sizes[1]))
    padded = (variables, rows + 4, cells + 2 * PAD, lanes)
    vmem = pl.BlockSpec(memory_space=pltpu.VMEM)
    dma = pltpu.SemaphoreType.DMA
    first, second, pull, table, mass, ends = pl.pallas_call(
        functools.partial(kernel, sizes, (slabs, wedges)),
        out_shape=(
            pltpu.VMEM(padded, jnp.float32),
            pltpu.VMEM(padded, jnp.float32),
            pltpu.VMEM((3 * TILE, lanes), jnp.float32),
            pltpu.VMEM((TILE, lanes), jnp.float32),
            pltpu.VMEM((1, rows), jnp.float32),
            pltpu.VMEM((2, variables, rows, lanes), jnp.float32),
        ),
        in_specs=[pl.BlockSpec(memory_space=pl.ANY)] * 3,
        out_specs=(vmem,) * 6,
        scratch_shapes=[
            *[pltpu.VMEM((2, variables, 2, rows, lanes), jnp.float32)] * 4,
            *[pltpu.VMEM((2, variables, 2, rows - 4, lanes), jnp.float32)] * 2,
            *[pltpu.VMEM((2, 2, variables, 2, 2, lanes), jnp.float32)] * 2,
            pltpu.VMEM((variables, rows + 1, cells, lanes), jnp.float32),
            pltpu.VMEM((1, lanes), jnp.float32),
            pltpu.VMEM((1, lanes), jnp.float32),
            pltpu.VMEM((wedges, 1, lanes), jnp.float32),
            pltpu.VMEM((slabs, 1, lanes), jnp.float32),
            pltpu.VMEM((1, lanes), jnp.float32),
            pltpu.SMEM((1,), jnp.float32),
            pltpu.SemaphoreType.REGULAR((2,)),
            pltpu.SemaphoreType.REGULAR,
            dma((3,)),
            dma((2,)),
            dma((4,)),
            dma((4,)),
            dma((4,)),
            dma((1,)),
            dma((1,)),
            dma((1,)),
            dma((1,)),
            dma((1,)),
        ],
        compiler_params=pltpu.CompilerParams(collective_id=0, has_side_effects=True),
    )(core_mass, table, conserved)
    advanced, mass = pl.pallas_call(
        functools.partial(finish, sizes),
        out_shape=(
            jax.ShapeDtypeStruct(conserved.shape, jnp.float32),
            jax.ShapeDtypeStruct((1, rows), jnp.float32),
        ),
        in_specs=[vmem] * 6,
        out_specs=(pl.BlockSpec(memory_space=pltpu.HBM),) * 2,
        scratch_shapes=[
            pltpu.VMEM(conserved.shape, jnp.float32),
            pltpu.VMEM((variables, rows + 1, cells, lanes), jnp.float32),
            dma((2,)),
        ],
        compiler_params=pltpu.CompilerParams(vmem_limit_bytes=16 * 1024 * 1024),
    )(first, second, pull, table, mass, ends)
    return advanced, mass.reshape(rows)


def solution(mesh):
    in_specs = (P(None, "radial", "phi", None), P())
    out_specs = (P(None, "radial", "phi", None), P("radial"))
    return jax.shard_map(body, mesh=mesh, in_specs=in_specs, out_specs=out_specs, check_vma=False)
```

```python
import functools
import math
import types

import jax
import jax.numpy as jnp
import numpy as np
from jax import lax
from jax.experimental import pallas as pl
from jax.experimental.pallas import tpu as pltpu
from jax.sharding import PartitionSpec as P

ADIABATIC = 4.0 / 3.0
INNER_RADIUS = 1.0
OUTER_RADIUS = 2.0
COURANT = 0.4
GRAVITY_KICK = 0.004
MINIMUM_DENSITY = 0.05
PRESSURE_FLOOR = 0.01
MESH = pl.DeviceIdType.MESH
TILE = 8
PAD = 8
DEPTH = 8
LINE = 2 * DEPTH
STEP = 4
TOP = 4


def step_sizes(radial_total, phi_total, theta_total):
    theta_step = math.pi / theta_total
    phi_step = 2.0 * math.pi / phi_total
    polar_width = INNER_RADIUS * math.sin(0.5 * theta_step) * phi_step
    radial_step = min(2.0 * polar_width, (OUTER_RADIUS - INNER_RADIUS) / radial_total)
    timestep = COURANT * min(radial_step, polar_width)
    return (radial_step, theta_step, phi_step, timestep)


def angle_tables(theta_cells, theta_step):
    step = np.float32(theta_step)
    centre = (np.arange(theta_cells, dtype=np.float32) + np.float32(0.5)) * step
    face = np.arange(theta_cells + 1, dtype=np.float32) * step
    sine = np.sin(centre.astype(np.float64))
    cosine = np.cos(centre.astype(np.float64))
    face_sine = np.sin(face.astype(np.float64))
    face_sine[-1] = 0.0
    zero = np.zeros(theta_cells)
    upper = 0.5 * face_sine[1:] / theta_step
    rows = [sine, upper, cosine / sine, 1.0 / sine, zero, zero, zero, zero]
    return np.stack(rows).astype(np.float32)


def half_slope(below, above):
    high, low = jnp.maximum(below, 0.0), jnp.minimum(below, 0.0)
    return 0.5 * jnp.maximum(jnp.minimum(above, high), low)


def thermo(q):
    density = jnp.maximum(q[0], MINIMUM_DENSITY)
    inverse = 1.0 / density
    kinetic = 0.5 * (q[1] * q[1] + q[2] * q[2] + q[3] * q[3]) * inverse
    pressure = jnp.maximum((ADIABATIC - 1.0) * (q[4] - kinetic), PRESSURE_FLOOR * density)
    return density, inverse, pressure


def physical(q, component):
    _, inverse, pressure = thermo(q)
    normal = q[component] * inverse
    squared = ADIABATIC * pressure * inverse
    return normal, pressure, jnp.abs(normal) + squared * lax.rsqrt(squared)


def flux(left, right, component, half_area):
    left_v, left_p, left_a = physical(left, component)
    right_v, right_p, right_a = physical(right, component)
    signal = jnp.maximum(left_a, right_a)
    left_w = half_area * (left_v + signal)
    right_w = half_area * (right_v - signal)
    out = [a * left_w + b * right_w for a, b in zip(left, right)]
    out[component] = out[component] + half_area * (left_p + right_p)
    out[4] = out[4] + half_area * (left_p * left_v + right_p * right_v)
    return out


def each(low, high, step):
    lax.fori_loop(low, high, lambda r, _: (step(r), 0)[1], 0)


def each_pair(low, high, step):
    def both(i):
        step(2 * i)
        step(2 * i + 1)

    each(low // 2, high // 2, both)


def stencils(sizes, extent, slab, table, ends, radial):
    radial_step, theta_step, phi_step, _ = sizes
    variables, rows, cells, lanes = extent
    tiles = cells // TILE
    shape = (TILE, lanes)
    sub = lax.broadcasted_iota(jnp.int32, shape, 0)
    lane_tile = lax.broadcasted_iota(jnp.int32, shape, 1)
    is_last = lane_tile == lanes - 1
    is_top, is_bottom = sub == TILE - 1, sub == 0

    def spread(value):
        return jnp.broadcast_to(value, shape)

    def radius_of(index):
        index = jnp.full(shape, slab * rows + index, jnp.int32).astype(jnp.float32)
        return INNER_RADIUS + (index + 0.5) * radial_step

    def radial_faces(buffer, low, count, tile):
        where = pl.ds(PAD + TILE * tile, TILE)
        lefts = [[] for _ in range(count)]
        rights = [[] for _ in range(count)]
        for k in range(variables):
            q = [buffer[k, low + j, where, :] for j in range(count + 3)]
            step = [q[j + 1] - q[j] for j in range(count + 2)]
            slope = [half_slope(step[j], step[j + 1]) for j in range(count + 1)]
            for i in range(count):
                lefts[i].append(q[i + 1] + slope[i])
                rights[i].append(q[i + 2] - slope[i + 1])
        out = []
        for i in range(count):
            face = radius_of(low + i) - 0.5 * radial_step
            out.append(flux(lefts[i], rights[i], 1, face * face * (0.5 / radial_step)))
        return out

    def radial_store(buffer, low, count):
        for t in range(tiles):
            for i, face in enumerate(radial_faces(buffer, low, count, t)):
                for k in range(variables):
                    radial[k, low + i, pl.ds(TILE * t, TILE), :] = face[k]

    def theta_part(centre):
        left, right = [], []
        for q in centre:
            after = pltpu.roll(q, lanes - 1, 1)
            above = jnp.where(is_last, 0.0, after - q)
            below = pltpu.roll(above, 1, 1)
            slope = half_slope(below, above)
            left.append(q + slope)
            right.append(pltpu.roll(q - slope, lanes - 1, 1))
        upper = flux(left, right, 2, spread(table[1:2, :]))
        return [pltpu.roll(f, 1, 1) - f for f in upper]

    def phi_ends(own, other, pulled):
        def column_at(k, buffer, side, cell):
            return pulled(k, side, cell, buffer is other, buffer[side, k, cell])

        left, right = [], []
        for k in range(variables):
            a, b = (column_at(k, other, 1, cell) for cell in range(2))
            c, d = (column_at(k, own, 0, cell) for cell in range(2))
            left.append(b + half_slope(b - a, c - b))
            right.append(c - half_slope(c - b, d - c))
            a = column_at(k, own, 1, 1)
            b, c = (column_at(k, other, 0, cell) for cell in range(2))
            ends[1, k] = b - half_slope(b - a, c - b)
        for k, f in enumerate(flux(left, right, 3, 0.5 / phi_step)):
            ends[0, k] = f

    def phi_part(buffer, r):
        left, right = [[] for _ in range(tiles)], [[] for _ in range(tiles)]
        for k in range(variables):
            turned = []
            for t in range(tiles):
                start = PAD + TILE * t
                a, b, c = (
                    buffer[k, r + 2, pl.ds(start + offset, TILE), :] for offset in (-1, 0, 1)
                )
                slope = half_slope(b - a, c - b)
                left[t].append(b + slope)
                turned.append(pltpu.roll(b - slope, TILE - 1, 0))
            turned.append(spread(ends[1, k, pl.ds(r, 1), :]))
            for t in range(tiles):
                right[t].append(jnp.where(is_top, turned[t + 1], turned[t]))
        upper = [flux(left[t], right[t], 3, 0.5 / phi_step) for t in range(tiles)]
        out = [[] for _ in range(tiles)]
        for k in range(variables):
            before = spread(ends[0, k, pl.ds(r, 1), :])
            for t in range(tiles):
                turned = pltpu.roll(upper[t][k], 1, 0)
                out[t].append(jnp.where(is_bottom, before, turned) - upper[t][k])
                before = turned
        return out

    def sources(centre, inverse_r):
        density, inverse, pressure = thermo(centre)
        vr, vt, vp = (centre[m] * inverse for m in (1, 2, 3))
        cot = spread(table[2:3, :])
        swirl = density * vp * vp
        return density, [
            (2.0 * pressure + density * vt * vt + swirl) * inverse_r,
            ((pressure + swirl) * cot - density * vr * vt) * inverse_r,
            -density * vp * (vr + vt * cot) * inverse_r,
        ]

    def centre_at(buffer, r, tile):
        return [
            buffer[k, r + 2, pl.ds(PAD + TILE * tile, TILE), :] for k in range(variables)
        ]

    return types.SimpleNamespace(
        spread=spread,
        radius_of=radius_of,
        radial_faces=radial_faces,
        radial_store=radial_store,
        theta_part=theta_part,
        phi_ends=phi_ends,
        phi_part=phi_part,
        sources=sources,
        centre_at=centre_at,
    )


def kernel(
    sizes,
    counts,
    core_ref,
    table_ref,
    input_ref,
    first,
    second,
    pull,
    table,
    mass_ref,
    ends,
    edge_one,
    halo_one,
    edge_two,
    halo_two,
    edge_inside,
    halo_inside,
    edge_end,
    halo_end,
    radial,
    part,
    slab_part,
    got_part,
    got,
    got_above,
    core,
    far,
    told,
    load_sem,
    radial_send,
    radial_recv,
    phi_send,
    phi_recv,
    part_send,
    part_recv,
    slab_send,
    slab_recv,
    above_recv,
):
    radial_step, theta_step, phi_step, timestep = sizes
    slabs, wedges = counts
    variables, rows, cells, lanes = input_ref.shape
    tiles = cells // TILE
    strength = GRAVITY_KICK / timestep
    slab, wedge = lax.axis_index("radial"), lax.axis_index("phi")
    has_up, has_down = slab < slabs - 1, slab > 0
    shape = (TILE, lanes)

    load = pltpu.make_async_copy(
        input_ref, first.at[:, pl.ds(2, rows), pl.ds(PAD, cells), :], load_sem.at[0]
    )
    load.start()
    load_table = pltpu.make_async_copy(table_ref, table, load_sem.at[1])
    load_table.start()
    load_core = pltpu.make_async_copy(core_ref, core, load_sem.at[2])
    load_core.start()

    def radial_peer(jump):
        return (slab + jump, wedge)

    def phi_peer(jump):
        return (slab, lax.rem(wedge + jump, wedges))

    barrier = pltpu.get_barrier_semaphore()
    x, z, c = slab // LINE, (slab // 2) % DEPTH, slab % 2
    level = jnp.where(z < TOP, z, TOP + x)
    rank = jnp.where(z < TOP, 2 * x + c, 2 * (z - TOP) + c)
    span, levels = slabs // DEPTH, DEPTH
    turns = jnp.logical_and(slab % LINE == 0, has_down)
    turned_last = slab % LINE == LINE - 1
    turned_to = jnp.logical_and(turned_last, has_up)

    def signal(semaphore, peer):
        pl.semaphore_signal(semaphore, inc=1, device_id=peer, device_id_type=MESH)

    def each_slab(low, high, step):
        def spread_out(at):
            for i in range(span):
                step(2 * at + LINE * (i // 2) + i % 2, False)

        def block(at):
            for i in range(span):
                last = i // 2 == DEPTH - TOP - 1
                step(LINE * at + (LINE // 2 - LINE * TOP + i), i % 2 == (1 if last else 0))

        each(low, jnp.minimum(high, TOP), spread_out)
        each(jnp.maximum(low, TOP), high, block)

    def greet(v):
        signal(barrier, (v, wedge))

    def near(v):
        return jnp.logical_or(v == slab + 1, v == slab - 1)

    def greet_level(v, later):
        known = jnp.logical_or(v < slab, v == slab + 1)
        known = jnp.logical_and(known, near(v)) if later else known
        pl.when(known)(lambda: greet(v))

    def greet_outer(v, later):
        if later:
            pl.when(near(v))(lambda: greet(v))
        else:
            greet(v)

    for j in range(1, wedges):
        signal(barrier, phi_peer(j))
    pl.when(jnp.logical_and(z > 0, jnp.logical_and(z <= TOP, c == 0)))(lambda: greet(slab - 1))
    pl.when(turned_to)(lambda: greet(slab + 1))
    each_slab(level, level + 1, greet_level)
    each_slab(level + 1, levels, greet_outer)
    inside = jnp.where(z < TOP, 2 * c, jnp.where(rank > 0, 1, 0))
    late = jnp.logical_and(z >= TOP, c == jnp.where(z == DEPTH - 1, 1, 0))
    inside = jnp.where(late, jnp.where(has_up, 2, 1), span * level + span - 1 - rank + inside)
    greeted = (wedges - 1) + inside + jnp.where(turns, 1, 0)
    further = slabs // LINE - 1 - x
    heard = (
        jnp.where(z < TOP, (TOP - 1 - z) * 2 * (further + 1), 0),
        jnp.where(z < TOP, (DEPTH - TOP) * 2 * (further + 1), span * further),
    )


    def remote(src, dst, send, recv, peer):
        return pltpu.make_async_remote_copy(
            src_ref=src, dst_ref=dst, send_sem=send, recv_sem=recv, device_id=peer,
            device_id_type=MESH,
        )

    def radial_copies(buffer, section):
        where, slot = pl.ds(PAD, cells), 2 * section
        up = remote(
            buffer.at[:, pl.ds(rows, 2), where, :], buffer.at[:, pl.ds(0, 2), where, :],
            radial_send.at[0], radial_recv.at[slot], radial_peer(1),
        )
        down = remote(
            buffer.at[:, pl.ds(2, 2), where, :], buffer.at[:, pl.ds(rows + 2, 2), where, :],
            radial_send.at[1], radial_recv.at[slot + 1], radial_peer(-1),
        )
        return up, down

    def radial_sent(copies):
        up, down = copies
        pl.when(has_up)(up.wait_send)
        pl.when(has_down)(down.wait_send)

    def radial_land(copies):
        up, down = copies
        pl.when(has_down)(up.wait_recv)
        pl.when(has_up)(down.wait_recv)

    def bottom_end(buffer):
        for t in range(tiles):
            where = pl.ds(PAD + TILE * t, TILE)
            value = buffer[:, 2, where, :]
            buffer[:, 0, where, :] = value
            buffer[:, 1, where, :] = value

    def top_end(buffer):
        for t in range(tiles):
            where = pl.ds(PAD + TILE * t, TILE)
            value = buffer[:, rows + 1, where, :]
            buffer[:, rows + 2, where, :] = value
            buffer[:, rows + 3, where, :] = value

    sides = ((0, PAD, PAD + cells, wedges - 1), (1, PAD + cells - 2, PAD - 2, 1))

    def phi_copies(source, target, slot):
        return [
            remote(
                source.at[side], target.at[side], phi_send.at[slot], phi_recv.at[slot],
                phi_peer(jump),
            )
            for side, _, _, jump in sides
        ]

    def phi_both(source, target, slot):
        return remote(source, target, phi_send.at[slot], phi_recv.at[slot], phi_peer(1))

    def phi_pack(buffer, full, piece, begin, count):
        for side, start, _, _ in sides:
            for i in range(count):
                value = buffer[:, 2 + begin + i, pl.ds(start, 2), :]
                piece[side, :, :, i, :] = value
                if full is not None:
                    full[side, :, :, begin + i, :] = value

    def phi_unpack(buffer, full, piece, begin, count):
        for side, _, start, _ in sides:
            for i in range(count):
                value = piece[side, :, :, i, :]
                buffer[:, 2 + begin + i, pl.ds(start, 2), :] = value
                if full is not None:
                    full[side, :, :, begin + i, :] = value

    first_radial, second_radial = radial_copies(first, 0), radial_copies(second, 1)
    load.wait()

    @pl.when(turned_last)
    def _():
        pl.semaphore_wait(barrier, greeted)
        pl.when(has_up)(first_radial[0].start)

    load_table.wait()
    load_core.wait()
    lane = lax.broadcasted_iota(jnp.int32, (rows, lanes), 1)
    line = lax.broadcasted_iota(jnp.int32, (rows, lanes), 0)
    column = jnp.sum(first[0, pl.ds(2, rows), pl.ds(PAD, cells), :], axis=1)
    column = jnp.sum(column * table[0:1, :], axis=1, keepdims=True)
    centres = INNER_RADIUS + (
        (slab * rows + line).astype(jnp.float32) + 0.5
    ) * radial_step
    column = column * centres * centres * (radial_step * theta_step * phi_step)
    part[...] = jnp.sum(jnp.where(lane == line, column, 0.0), axis=0, keepdims=True)

    on = stencils(sizes, input_ref.shape, slab, table, ends, radial)

    def early_one(r):
        inverse_r = 1.0 / on.radius_of(r)
        around = inverse_r * on.spread(table[3:4, :]) * timestep
        for t in range(tiles):
            centre = on.centre_at(first, r, t)
            total = [c + d * around for c, d in zip(centre, on.theta_part(centre))]
            _, source = on.sources(centre, inverse_r)
            for m in range(3):
                total[m + 1] = total[m + 1] + timestep * source[m]
            for k in range(variables):
                second[k, r + 2, pl.ds(PAD + TILE * t, TILE), :] = total[k]

    def late_one(r):
        inverse_r = 1.0 / on.radius_of(r)
        around = inverse_r * on.spread(table[3:4, :]) * timestep
        along = inverse_r * inverse_r * timestep
        for t, part_of in enumerate(on.phi_part(first, r)):
            into = pl.ds(TILE * t, TILE)
            where = pl.ds(PAD + TILE * t, TILE)
            for k in range(variables):
                across = radial[k, r, into, :] - radial[k, r + 1, into, :]
                second[k, r + 2, where, :] = (
                    second[k, r + 2, where, :] + part_of[k] * around + across * along
                )

    pl.when(jnp.logical_not(turned_last))(lambda: pl.semaphore_wait(barrier, greeted))

    def reply(v, _):
        pl.when(v < slab)(lambda: signal(far.at[jnp.where(z < TOP, 0, 1)], (v, wedge)))

    part_copies = [
        remote(part, got_part.at[j], part_send.at[0], part_recv.at[0], phi_peer(j))
        for j in range(1, wedges)
    ]
    others = pl.ds(1, wedges - 1)
    part_all = remote(
        got_part.at[others], got_part.at[others], part_send.at[0], part_recv.at[0], phi_peer(1)
    )
    first_phi = phi_copies(edge_one, halo_one, 0)
    inside_phi = phi_copies(edge_inside, halo_inside, 1)
    for copy in part_copies:
        copy.start()
    phi_pack(first, None, edge_one, 0, rows)
    pl.when(jnp.logical_and(has_up, jnp.logical_not(turned_last)))(first_radial[0].start)
    pl.when(has_down)(first_radial[1].start)
    for copy in first_phi:
        copy.start()

    teller = jnp.logical_and(z >= TOP, jnp.logical_not(late))
    pl.when(teller)(lambda: signal(told, (slab + 1 - 2 * c, wedge)))

    @pl.when(jnp.logical_not(late))
    def _():
        each_slab(0, level, reply)

    got_part[0] = part[...]
    each_pair(0, rows, early_one)

    @pl.when(late)
    def _():
        pl.semaphore_wait(told, 1)
        each_slab(0, level, reply)

    each(0, 2, lambda i: on.radial_store(first, 2 + 2 * i, 2))
    on.radial_store(first, 6, 1)
    part_all.wait_recv()
    shells = jnp.zeros((1, lanes), jnp.float32)
    for w in range(wedges):
        shells = shells + got_part[lax.rem(wedge + wedges - w, wedges)]
    slab_part[...] = shells

    def slab_copy(source, target):
        return remote(
            slab_part, got.at[source], slab_send.at[0], slab_recv.at[0], (target, wedge),
        )

    def slab_all(count):
        ref = got.at[pl.ds(0, count)]
        return remote(ref, ref, slab_send.at[0], slab_recv.at[0], radial_peer(0))

    def by_slab(low, high, step):
        if high - low == 1:
            step(low)
            return
        middle = (low + high) // 2
        pl.when(slab < middle)(lambda: by_slab(low, middle, step))
        pl.when(slab >= middle)(lambda: by_slab(middle, high, step))

    def slab_start(v, _):
        pl.when(v > slab)(lambda: slab_copy(slab, v).start())

    above_copy = remote(
        slab_part, got_above, slab_send.at[0], above_recv.at[0], radial_peer(-1)
    )
    each_slab(0, level + 1, slab_start)
    pl.when(has_down)(above_copy.start)

    def send_out():
        for at, low, high in ((0, level + 1, TOP), (1, jnp.maximum(level + 1, TOP), levels)):
            @pl.when(heard[at] > 0)
            def _():
                pl.semaphore_wait(far.at[at], heard[at])
                each_slab(low, high, slab_start)

    def edge_rows(number, high):
        up, down = first_radial
        second_up, second_down = second_radial
        begin = jnp.where(high, rows - 2, 0)
        low = jnp.logical_not(high)
        pl.when(jnp.logical_and(high, has_up))(down.wait_recv)
        pl.when(jnp.logical_and(low, has_down))(up.wait_recv)
        pl.when(jnp.logical_and(high, jnp.logical_not(has_up)))(lambda: top_end(first))
        pl.when(jnp.logical_and(low, jnp.logical_not(has_down)))(lambda: bottom_end(first))
        on.radial_store(first, jnp.where(high, rows - 1, 0), 2)
        each(begin, begin + 2, late_one)

        @pl.when(jnp.logical_and(high, has_up))
        def _():
            up.wait_send()
            second_up.start()

        @pl.when(jnp.logical_and(low, has_down))
        def _():
            down.wait_send()
            second_down.start()

        phi_pack(second, edge_two, edge_end.at[number], begin, 2)
        for copy in phi_copies(edge_end.at[number], halo_end.at[number], 2 + number):
            copy.start()

    phi_both(edge_one, halo_one, 0).wait_recv()
    phi_unpack(first, None, halo_one, 0, rows)
    on.phi_ends(edge_one, halo_one, lambda k, side, cell, other, value: value)
    each(2, rows - 2, late_one)
    phi_pack(second, edge_two, edge_inside, 2, rows - 4)
    for copy in inside_phi:
        copy.start()
    edge_rows(0, c == 0)
    edge_rows(1, c == 1)
    send_out()

    after = jnp.where(lane < line, 1.0, jnp.where(lane == line, 0.5, 0.0))
    within = jnp.sum(after * slab_part[...], axis=1, keepdims=True)
    whole = jnp.sum(jnp.where(line >= 0, slab_part[...], 0.0), axis=1, keepdims=True)

    phi_both(edge_inside, halo_inside, 1).wait_recv()
    phi_unpack(second, halo_two, halo_inside, 2, rows - 4)
    for number in range(2):
        begin = jnp.where(c == number, rows - 2, 0)
        phi_both(edge_end.at[number], halo_end.at[number], 2 + number).wait_recv()
        phi_unpack(second, halo_two, halo_end.at[number], begin, 2)
    radial_land(second_radial)

    part_all.wait_send()
    phi_both(edge_one, halo_one, 0).wait_send()
    phi_both(edge_inside, halo_inside, 1).wait_send()
    for number in range(2):
        phi_both(edge_end.at[number], halo_end.at[number], 2 + number).wait_send()
    radial_sent(second_radial)
    by_slab(0, slabs, lambda s: slab_all(slabs - max(s, 1)).wait_send())
    pl.when(has_up)(above_copy.wait_recv)
    by_slab(0, slabs, lambda s: slab_all(s).wait_recv() if s else None)
    sums = [jnp.zeros((1, lanes), jnp.float32) for _ in range(4)]
    for v in range(slabs - 1):
        sums[v % 4] = sums[v % 4] + jnp.where(slab > v, got[v], 0.0)
    before = jnp.broadcast_to((sums[0] + sums[1]) + (sums[2] + sums[3]), (rows, lanes))
    before = core[0] + jnp.sum(before, axis=1, keepdims=True)
    inner = jnp.where(lane > line, 1.0, jnp.where(lane == line, 0.5, 0.0))
    inner = jnp.sum(inner * got[jnp.maximum(slab - 1, 0)], axis=1, keepdims=True)
    outer = jnp.sum(after * got_above[...], axis=1, keepdims=True)
    wide = jnp.zeros((rows, lanes), jnp.float32)
    enclosed = before + within + wide
    mass_ref[...] = jnp.sum(jnp.where(lane == line, enclosed, 0.0), axis=0, keepdims=True)[:, :rows]
    for i, inside in ((0, before - inner), (1, before + within), (2, before + whole + outer)):
        at = centres + (i - 1) * rows * radial_step
        pull[pl.ds(8 * i, 8), :] = strength * (inside + wide) / (at * at)

    def pulled(row, start):
        where = pl.ds(start, TILE)
        gravity = timestep * on.spread(pull[pl.ds(row + 6, 1), :])
        density = jnp.maximum(first[0, row, where, :], MINIMUM_DENSITY)
        second[1, row, where, :] = second[1, row, where, :] - density * gravity
        second[4, row, where, :] = second[4, row, where, :] - first[1, row, where, :] * gravity

    def pulled_row(row):
        for t in range(-1, tiles + 1):
            pulled(row, PAD + TILE * t)

    each_pair(0, rows + 4, pulled_row)
    pl.when(jnp.logical_not(has_down))(lambda: bottom_end(second))
    pl.when(jnp.logical_not(has_up))(lambda: top_end(second))

    tug = timestep * pull[pl.ds(TILE, rows), :]

    def pulled_end(k, side, cell, other, value):
        begin = halo_one if other else edge_one
        if k == 1:
            value = value - jnp.maximum(begin[side, 0, cell], MINIMUM_DENSITY) * tug
        if k == 4:
            value = value - begin[side, 1, cell] * tug
        return value

    on.phi_ends(edge_two, halo_two, pulled_end)


def finish(
    sizes,
    first,
    second,
    pull,
    table,
    mass,
    ends,
    out_ref,
    mass_ref,
    out,
    radial,
    sem,
):
    timestep = sizes[3]
    variables, rows, cells, lanes = out.shape
    tiles = cells // TILE
    slab = lax.axis_index("radial")
    on = stencils(sizes, out.shape, slab, table, ends, radial)
    save_mass = pltpu.make_async_copy(mass, mass_ref, sem.at[1])
    save_mass.start()

    def section_two(r):
        inverse_r = 1.0 / on.radius_of(r)
        scale = 0.5 * timestep
        around = inverse_r * on.spread(table[3:4, :]) * scale
        along = inverse_r * inverse_r * scale
        gravity = on.spread(pull[pl.ds(r + 8, 1), :])
        phi = on.phi_part(second, r)
        for t in range(tiles):
            into = pl.ds(TILE * t, TILE)
            where = pl.ds(PAD + TILE * t, TILE)
            centre = on.centre_at(second, r, t)
            theta = on.theta_part(centre)
            density, source = on.sources(centre, inverse_r)
            source[0] = source[0] - density * gravity
            source.append(-centre[1] * gravity)
            total = [
                0.5 * (first[k, r + 2, where, :] + centre[k])
                + (theta[k] + phi[t][k]) * around
                + (radial[k, r, into, :] - radial[k, r + 1, into, :]) * along
                for k in range(variables)
            ]
            for m in range(4):
                total[m + 1] = total[m + 1] + scale * source[m]
            for k in range(variables):
                out[k, r, into, :] = total[k]

    def save(i):
        where = (slice(None), pl.ds(STEP * i, STEP))
        return pltpu.make_async_copy(out.at[where], out_ref.at[where], sem.at[0])

    def several(i):
        for j in range(STEP):
            section_two(STEP * i + j)
        save(i).start()

    for i in range((rows + 1) // 3):
        on.radial_store(second, 3 * i, 3)
    each(0, rows // STEP, several)
    pltpu.make_async_copy(out, out_ref, sem.at[0]).wait()
    save_mass.wait()


def body(conserved, core_mass):
    variables, rows, cells, lanes = conserved.shape
    slabs, wedges = lax.axis_size("radial"), lax.axis_size("phi")
    sizes = step_sizes(rows * slabs, cells * wedges, lanes)
    table = jnp.asarray(angle_tables(lanes, sizes[1]))
    padded = (variables, rows + 4, cells + 2 * PAD, lanes)
    vmem = pl.BlockSpec(memory_space=pltpu.VMEM)
    dma = pltpu.SemaphoreType.DMA
    first, second, pull, table, mass, ends = pl.pallas_call(
        functools.partial(kernel, sizes, (slabs, wedges)),
        out_shape=(
            pltpu.VMEM(padded, jnp.float32),
            pltpu.VMEM(padded, jnp.float32),
            pltpu.VMEM((3 * TILE, lanes), jnp.float32),
            pltpu.VMEM((TILE, lanes), jnp.float32),
            pltpu.VMEM((1, rows), jnp.float32),
            pltpu.VMEM((2, variables, rows, lanes), jnp.float32),
        ),
        in_specs=[pl.BlockSpec(memory_space=pl.ANY)] * 3,
        out_specs=(vmem,) * 6,
        scratch_shapes=[
            *[pltpu.VMEM((2, variables, 2, rows, lanes), jnp.float32)] * 4,
            *[pltpu.VMEM((2, variables, 2, rows - 4, lanes), jnp.float32)] * 2,
            *[pltpu.VMEM((2, 2, variables, 2, 2, lanes), jnp.float32)] * 2,
            pltpu.VMEM((variables, rows + 1, cells, lanes), jnp.float32),
            pltpu.VMEM((1, lanes), jnp.float32),
            pltpu.VMEM((1, lanes), jnp.float32),
            pltpu.VMEM((wedges, 1, lanes), jnp.float32),
            pltpu.VMEM((slabs, 1, lanes), jnp.float32),
            pltpu.VMEM((1, lanes), jnp.float32),
            pltpu.SMEM((1,), jnp.float32),
            pltpu.SemaphoreType.REGULAR((2,)),
            pltpu.SemaphoreType.REGULAR,
            dma((3,)),
            dma((2,)),
            dma((4,)),
            dma((4,)),
            dma((4,)),
            dma((1,)),
            dma((1,)),
            dma((1,)),
            dma((1,)),
            dma((1,)),
        ],
        compiler_params=pltpu.CompilerParams(collective_id=0, has_side_effects=True),
    )(core_mass, table, conserved)
    advanced, mass = pl.pallas_call(
        functools.partial(finish, sizes),
        out_shape=(
            jax.ShapeDtypeStruct(conserved.shape, jnp.float32),
            jax.ShapeDtypeStruct((1, rows), jnp.float32),
        ),
        in_specs=[vmem] * 6,
        out_specs=(pl.BlockSpec(memory_space=pltpu.HBM),) * 2,
        scratch_shapes=[
            pltpu.VMEM(conserved.shape, jnp.float32),
            pltpu.VMEM((variables, rows + 1, cells, lanes), jnp.float32),
            dma((2,)),
        ],
        compiler_params=pltpu.CompilerParams(vmem_limit_bytes=16 * 1024 * 1024),
    )(first, second, pull, table, mass, ends)
    return advanced, mass.reshape(rows)


def solution(mesh):
    in_specs = (P(None, "radial", "phi", None), P())
    out_specs = (P(None, "radial", "phi", None), P("radial"))
    return jax.shard_map(body, mesh=mesh, in_specs=in_specs, out_specs=out_specs, check_vma=False)
```
